128 devices in a mesh: lat: 8 (over z, core), lon: 16 (over y, x).
Axes of the slice: x: 4, y: 4, z: 4, core: 2. Of those that a mesh axis runs over, the one named last changes fastest.
Arguments:
- zonal_wind: float32 [32, 64, 2048], P(None, 'lat', 'lon'), may hold values from -6 to 6
- merid_wind: float32 [32, 64, 2048], P(None, 'lat', 'lon'), may hold values from -6 to 6
- vertical_wind: float32 [32, 64, 2048], P(None, 'lat', 'lon'), may hold values from -6 to 6
- pressure: float32 [32, 64, 2048], P(None, 'lat', 'lon'), may hold values from -6 to 6
- zonal_coef: float32 [64], P('lat'), may hold values from 0.05 to 0.4
- merid_coef: float32 [64], P('lat'), may hold values from 0.05 to 0.4
- level_coef: float32 [32], replicated, may hold values from 0.3 to 1.5
- sound_coef: float32 [32, 64, 2048], P(None, 'lat', 'lon'), may hold values from 0.2 to 2
- cutoff: int32 [64], replicated, may hold values from 1 to 511
- filter_mask: int32 [64], replicated, may hold values from 0 to 1, as said below
Outputs:
- zonal_next: float32 [32, 64, 2048], P(None, 'lat', 'lon')
- merid_next: float32 [32, 64, 2048], P(None, 'lat', 'lon')
- vertical_next: float32 [32, 64, 2048], P(None, 'lat', 'lon')
- pressure_next: float32 [32, 64, 2048], P(None, 'lat', 'lon')
The draws below stay inside these ranges and needn't reach their ends.
Inputs may be any that keep to these rules, and one draw needn't show every extreme that they name: `filter_mask`: for every latitude j below 32 exactly one of j and j + 32 is filtered; the filtered ones are the first n and the last 32 - n latitudes, for some n from 8 to 24.
All inputs are finite; a program needn't handle non-finite values.
Results may differ from the reference program's by a relative error of at most 0.0001.
Values sent between devices are 32-bit elements; how exact they have to be, the bound alone decides.
A program may use at most 64 MiB of HBM per device.

```python
import math
import jax
import jax.numpy as jnp
from jax import lax

NLON = 2048
NLEV = 32
SUBSTEPS = 2
NLAT = 64


def draw_filter_mask(key, part):
    latitudes = jnp.arange(NLAT)
    northern = jax.random.randint(jax.random.fold_in(key, 17), (), NLAT // 8, 3 * NLAT // 8 + 1)
    southern_start = NLAT // 2 + northern
    return jnp.logical_or(latitudes < northern, latitudes >= southern_start).astype(jnp.int32)


def set_ends(drawn, own_key, smallest, top_value):
    place = [jax.random.randint(jax.random.fold_in(own_key, axis), (), 0, length) for axis, length in enumerate(drawn.shape)]
    widest = drawn.shape.index(max(drawn.shape))
    beside = place[:widest] + [(place[widest] + 1) % drawn.shape[widest]] + place[widest + 1:]
    return drawn.at[tuple(place)].set(smallest).at[tuple(beside)].set(top_value)


def block_scale(stream_key, extent, cuts, low, top_value):
    level = 1.0
    for position, parts in cuts:
        draws = jax.random.uniform(jax.random.fold_in(jax.random.fold_in(stream_key, 6), position), (parts,), jnp.float32, low / len(cuts), top_value / len(cuts))
        level = level * jnp.repeat(jnp.exp(draws), extent[position] // parts).reshape((-1,) + (1,) * (len(extent) - 1 - position))
    return level


def noise(own_key, dims, deviation, reach, shards=(), dtype=jnp.bfloat16):
    entries = deviation * jax.random.normal(own_key, dims, jnp.float32)
    if shards:
        entries = entries * block_scale(own_key, dims, shards, -0.22, 0.18)
    return jnp.clip(entries, -reach, reach).astype(dtype)


def setup_inputs(seed: int = 0) -> dict:
    streams_of = jax.random.split(jax.random.key(seed), 11)
    return {
        "zonal_wind": noise(streams_of[0], (NLEV, NLAT, NLON), 1.0, 6.0, ((1, 8), (2, 16)), jnp.float32),
        "merid_wind": noise(streams_of[1], (NLEV, NLAT, NLON), 1.0, 6.0, ((1, 8), (2, 16)), jnp.float32),
        "vertical_wind": noise(streams_of[2], (NLEV, NLAT, NLON), 1.0, 6.0, ((1, 8), (2, 16)), jnp.float32),
        "pressure": noise(streams_of[3], (NLEV, NLAT, NLON), 1.0, 6.0, ((1, 8), (2, 16)), jnp.float32),
        "zonal_coef": jnp.clip(jnp.exp(math.log(0.4) - 2.0794415 * jax.random.uniform(streams_of[4], (NLAT,), jnp.float32) ** block_scale(streams_of[4], (NLAT,), ((0, 8),), -0.2, 0.2)), 0.05, 0.4),
        "merid_coef": jnp.clip(jnp.exp(math.log(0.4) - 2.0794415 * jax.random.uniform(streams_of[5], (NLAT,), jnp.float32) ** block_scale(streams_of[5], (NLAT,), ((0, 8),), -0.2, 0.2)), 0.05, 0.4),
        "level_coef": jnp.clip(jnp.exp(jax.random.uniform(streams_of[6], (NLEV,), jnp.float32, math.log(0.3), math.log(1.5))), 0.3, 1.5),
        "sound_coef": jnp.clip(jnp.exp(math.log(2.0) - 2.3025851 * jax.random.uniform(streams_of[7], (NLEV, NLAT, NLON), jnp.float32) ** block_scale(streams_of[7], (NLEV, NLAT, NLON), ((1, 8), (2, 16)), -0.2, 0.2)), 0.2, 2.0),
        "cutoff": set_ends(jax.random.randint(streams_of[8], (NLAT,), 1, NLON // 4), jax.random.fold_in(streams_of[8], 1), 1, (NLON // 4) - 1).astype(jnp.int32),
        "filter_mask": draw_filter_mask(jax.random.fold_in(streams_of[10], 71), 0),
    }


def zonal_diff(field):
    return jnp.roll(field, -1, axis=2) - jnp.roll(field, 1, axis=2)


def merid_diff(field):
    padded = jnp.pad(field, ((0, 0), (1, 1), (0, 0)))
    return padded[:, 2:, :] - padded[:, :-2, :]


def damping(wavenum, limits):
    bound_col = limits[:, None]
    ratio = bound_col / jnp.maximum(wavenum[None, :], 1.0)
    return jnp.where(wavenum[None, :] > bound_col, ratio * ratio, 1.0)


def polar_damp(field, cutoff, filter_mask):
    wavenum = jnp.arange(NLON // 2 + 1).astype(jnp.float32)
    factor = damping(wavenum, cutoff.astype(jnp.float32))

    def one_level(slab):
        spectra = jnp.fft.rfft(slab, axis=1)
        return jnp.fft.irfft(spectra * factor, n=NLON, axis=1).astype(jnp.float32)

    damped = lax.map(one_level, field)
    return jnp.where(filter_mask[None, :, None] > 0, damped, field)


def column_solve(vertical_wind, pstar, level_coef, sound_coef):
    levels = vertical_wind.shape[0]
    zero_slab = jnp.zeros_like(vertical_wind[0])
    ratios = []
    values = []
    prev_ratio = zero_slab
    prev_value = zero_slab
    for level in range(levels):
        alpha = level_coef[level]
        below = alpha * sound_coef[level]
        if level + 1 < levels:
            above = alpha * sound_coef[level + 1]
            rhs = vertical_wind[level] - alpha * (pstar[level + 1] - pstar[level])
        else:
            above = zero_slab
            rhs = vertical_wind[level] + alpha * pstar[level]
        pivot = 1.0 + below + above + below * prev_ratio
        prev_ratio = -above / pivot
        prev_value = (rhs + below * prev_value) / pivot
        ratios.append(prev_ratio)
        values.append(prev_value)
    solved = [zero_slab] * levels
    upper_value = values[levels - 1]
    solved[levels - 1] = upper_value
    for level in range(levels - 2, -1, -1):
        upper_value = values[level] - ratios[level] * upper_value
        solved[level] = upper_value
    new_wind = jnp.stack(solved)
    wind_below = jnp.concatenate([zero_slab[None], new_wind[:-1]], axis=0)
    new_pressure = pstar - sound_coef * (new_wind - wind_below)
    return new_wind, new_pressure


def reference(zonal_wind, merid_wind, vertical_wind, pressure, zonal_coef, merid_coef, level_coef, sound_coef, cutoff, filter_mask):
    zonal_rows = zonal_coef[None, :, None]
    merid_rows = merid_coef[None, :, None]
    for step in range(SUBSTEPS):
        zonal_step = -zonal_rows * zonal_diff(pressure)
        merid_step = -merid_rows * merid_diff(pressure)
        zonal_wind = zonal_wind + polar_damp(zonal_step, cutoff, filter_mask)
        merid_wind = merid_wind + polar_damp(merid_step, cutoff, filter_mask)
        diverge = zonal_rows * zonal_diff(zonal_wind) + merid_rows * merid_diff(merid_wind)
        pstar = pressure - sound_coef * diverge
        vertical_wind, pressure = column_solve(vertical_wind, pstar, level_coef, sound_coef)
    return (zonal_wind, merid_wind, vertical_wind, pressure)
```

```python
import math

import jax
import jax.numpy as jnp
import numpy as np
from jax import lax
from jax.experimental import pallas as pl
from jax.experimental.pallas import tpu as pltpu
from jax.sharding import PartitionSpec as P

SUBSTEPS = 2
F32 = jnp.float32
NG = 8
ND = 16
NL = 32
MESH = pl.DeviceIdType.MESH


def tables():
    lane = np.arange(128)
    ang = 2.0 * np.pi * ((lane[:, None] * lane[None, :]) % 128) / 128.0
    c, s = np.cos(ang), np.sin(ang)
    mat = np.block([[c, -s], [s, c]]).astype(np.float32)
    tang = 2.0 * np.pi * (np.arange(16)[:, None] * lane[None, :]) / 2048.0
    tw = np.stack([np.cos(tang), -np.sin(tang)]).astype(np.float32)
    return mat, tw


def dft4(x):
    (ar, ai), (br, bi), (cr, ci), (dr, di) = x
    sr, si = ar + cr, ai + ci
    tr, ti = ar - cr, ai - ci
    ur, ui = br + dr, bi + di
    vr, vi = br - dr, bi - di
    return [(sr + ur, si + ui), (tr + vi, ti - vr), (sr - ur, si - ui), (tr - vi, ti + vr)]


def dft16(x):
    cols = []
    for n2 in range(4):
        y = dft4([x[4 * n1 + n2] for n1 in range(4)])
        out = []
        for k1 in range(4):
            e = (n2 * k1) % 16
            yr, yi = y[k1]
            if e == 0:
                out.append((yr, yi))
            elif e == 4:
                out.append((yi, -yr))
            else:
                c, s = math.cos(2 * math.pi * e / 16), math.sin(2 * math.pi * e / 16)
                out.append((yr * c + yi * s, yi * c - yr * s))
        cols.append(out)
    res = [None] * 16
    for k1 in range(4):
        z = dft4([cols[n2][k1] for n2 in range(4)])
        for k2 in range(4):
            res[k1 + 4 * k2] = z[k2]
    return res


def hops(off):
    return sum(min(o, 4 - o) for o in off)


OFFS = sorted([(a, b) for a in range(4) for b in range(4)], key=lambda o: -hops(o))


def kernel(
    zc_s, mc_s, a_s, cut_s, msk_s, u_h, v_h, w_h, p_h, s_h, mat_h, tw_h,
    uo_h, vo_h, wo_h, po_h,
    uv, vv, wv, pv, sv, mat, tw, p1, w1, p2, w2, xm, xe, bs, hs, lhs, res, dsend, back,
    du, dv, ru, rv, rat, inv, qq, div0, eu, eul, eur, ev, mct, mcp, mcn, fo, fh,
    ldsem, outsem, sendsem, fmsem, fesem, bksem, esem,
):
    me = lax.axis_index("lon")
    g = lax.axis_index("lat")
    up = (g + 1) % NG
    dn = (g + NG - 1) % NG
    my, mx = me // 4, me % 4
    east = (me + 1) % ND
    west = (me + ND - 1) % ND

    loads = [
        pltpu.make_async_copy(a, b, ldsem.at[i])
        for i, (a, b) in enumerate(
            [(p_h, pv), (u_h, uv), (v_h, vv), (s_h, sv), (w_h, wv), (tw_h, tw), (mat_h, mat)]
        )
    ]
    for c in loads:
        c.start()

    bar = pltpu.get_barrier_semaphore()

    def target(off):
        return ((my + off[0]) % 4) * 4 + (mx + off[1]) % 4

    for off in OFFS:
        d = target(off)
        pl.semaphore_signal(bar, inc=1, device_id={"lat": up, "lon": d}, device_id_type=MESH)
        pl.semaphore_signal(bar, inc=1, device_id={"lat": dn, "lon": d}, device_id_type=MESH)
        if off != (0, 0):
            pl.semaphore_signal(bar, inc=1, device_id={"lat": g, "lon": d}, device_id_type=MESH)

    def rcopy(src, dst, si, sem, gg, d):
        c = pltpu.make_async_remote_copy(
            src_ref=src, dst_ref=dst, send_sem=sendsem.at[si], recv_sem=sem,
            device_id={"lat": gg, "lon": d}, device_id_type=MESH,
        )
        c.start()

    def forward(ph, src):
        for off in OFFS:
            d = target(off)
            if off != (0, 0):
                rcopy(src.at[pl.ds(2 * d, 2)], xm.at[ph, me], 3 * ph, fmsem.at[ph], g, d)
            rcopy(src.at[pl.ds(2 * d, 2), 6:8], xe.at[ph, me, :, 6:8], 3 * ph + 1, fesem.at[ph, 0], up, d)
            rcopy(src.at[pl.ds(2 * d, 2), 0:2], xe.at[ph, me, :, 0:2], 3 * ph + 2, fesem.at[ph, 1], dn, d)
        xm[ph, pl.ds(me, 1)] = src[pl.ds(2 * me, 2)][None]

    def wait15(buf, sem):
        pltpu.make_async_copy(buf.at[pl.ds(0, 15)], buf.at[pl.ds(0, 15)], sem).wait()

    def wait_all(buf, sem):
        pltpu.make_async_copy(buf, buf, sem).wait()

    sub = lax.broadcasted_iota(jnp.int32, (8, 128), 0)
    lane = lax.broadcasted_iota(jnp.int32, (8, 128), 1)

    def tile(read):
        t = jnp.full((8, 128), read(0))
        for r in range(1, 8):
            t = jnp.where(sub == r, read(r), t)
        return t

    zc = tile(lambda r: zc_s[r])
    mc = tile(lambda r: mc_s[r])
    mct[...] = mc
    own = lambda ref: tile(lambda r: ref[8 * g + r])
    halo = lambda ref: jnp.where(sub == 0, ref[(8 * g + 8) % 64], ref[(8 * g + 63) % 64])
    keep_o = own(msk_s) > 0
    keep_h = halo(msk_s) > 0
    valid = jnp.logical_or(
        jnp.logical_and(sub >= 4, jnp.full((8, 128), g) > 0),
        jnp.logical_and(sub < 4, jnp.full((8, 128), g) < NG - 1),
    )

    loads[0].wait()
    pl.semaphore_wait(bar, 47)
    forward(0, pv)
    rcopy(mct, mcp, 6, esem.at[0], up, me)
    rcopy(mct, mcn, 6, esem.at[1], dn, me)
    loads[1].wait()
    e = jnp.zeros((8, 128), F32)
    for k in range(NL):
        uk = uv[k]
        e = jnp.where(lane == k, pltpu.roll(uk, (k + 1) % 128, 1), e)
        e = jnp.where(lane == 32 + k, pltpu.roll(uk, 32 + k, 1), e)
    eu[...] = e
    rcopy(eu, eul, 7, esem.at[2], g, east)
    rcopy(eu, eur, 7, esem.at[3], g, west)
    loads[2].wait()
    rcopy(vv.at[:, 7:8], ev.at[:, 7:8], 8, esem.at[4], up, me)
    rcopy(vv.at[:, 0:1], ev.at[:, 0:1], 9, esem.at[5], dn, me)

    def factors(cut):
        k1 = lax.broadcasted_iota(jnp.int32, (16, 8, 128), 0)
        k2 = lax.broadcasted_iota(jnp.int32, (16, 8, 128), 2)
        k = k1 + 16 * k2
        kk = jnp.minimum(k, 2048 - k).astype(F32)
        c = cut.astype(F32)[None]
        ratio = c / jnp.maximum(kk, 1.0)
        f = jnp.where(kk > c, ratio * ratio, 1.0) * (1.0 / 2048.0)
        return f.reshape(128, 128)

    fo[...] = factors(own(cut_s))
    fh[...] = factors(halo(cut_s))

    loads[3].wait()
    prev = jnp.zeros((8, 128), F32)
    for k in range(NL):
        al = a_s[k]
        below = al * sv[k]
        above = al * sv[k + 1] if k + 1 < NL else jnp.zeros((8, 128), F32)
        ip = 1.0 / (1.0 + below + above + below * prev)
        prev = -above * ip
        rat[k] = prev
        inv[k] = ip
        qq[k] = below * ip

    wait_all(mcp, esem.at[0])
    wait_all(mcn, esem.at[1])
    mch = jnp.where(sub >= 4, mcp[...], mcn[...])
    mch = jnp.where(valid, mch, 0.0)
    wait_all(eul, esem.at[2])
    wait_all(eur, esem.at[3])
    wait_all(ev.at[:, 7:8], esem.at[4])
    wait_all(ev.at[:, 0:1], esem.at[5])
    el, er = eul[...], eur[...]
    for k in range(NL):
        uk, vk = uv[k], vv[k]
        evk = jnp.where(valid, ev[k], 0.0)
        right = jnp.where(lane == 127, pltpu.roll(er, (95 - k) % 128, 1), pltpu.roll(uk, 127, 1))
        left = jnp.where(lane == 0, pltpu.roll(el, (128 - k) % 128, 1), pltpu.roll(uk, 1, 1))
        north = pltpu.roll(jnp.where(sub == 0, evk, vk), 7, 0)
        south = pltpu.roll(jnp.where(sub == 7, evk, vk), 1, 0)
        div0[k] = zc * (right - left) + mc * (north - south)

    loads[4].wait()
    loads[5].wait()
    loads[6].wait()

    def get_main(ph, d, l):
        x = xm[0, d, l]
        return x + xm[1, d, l] if ph else x

    def get_edge(ph, d, l):
        x = xe[0, d, l]
        x = x + xe[1, d, l] if ph else x
        return jnp.where(valid, x, 0.0)

    def store_spec(t, spec):
        for k1 in range(16):
            r, i = spec[k1]
            tr, ti = tw[0, k1 : k1 + 1, :], tw[1, k1 : k1 + 1, :]
            row = t * 128 + k1 * 8
            lhs[row : row + 8, 0:128] = r * tr - i * ti
            lhs[row : row + 8, 128:256] = r * ti + i * tr

    def big_dot(x):
        return jnp.dot(x, mat[...], precision=lax.Precision.HIGHEST, preferred_element_type=F32)

    def unfold(t):
        x = []
        for k1 in range(16):
            row = t * 128 + k1 * 8
            r, i = res[row : row + 8, 0:128], res[row : row + 8, 128:256]
            tr, ti = tw[0, k1 : k1 + 1, :], tw[1, k1 : k1 + 1, :]
            x.append((r * tr - i * ti, r * ti + i * tr))
        return [(b, a) for a, b in dft16(x)]

    def level_part(ph):
        wait15(xm.at[ph], fmsem.at[ph])
        wait_all(xe.at[ph, :, :, 0:2], fesem.at[ph, 0])
        wait_all(xe.at[ph, :, :, 0:2], fesem.at[ph, 1])
        for l in range(2):
            z = []
            for d in range(16):
                x, ee = get_main(ph, d, l), get_edge(ph, d, l)
                xu, xd = pltpu.roll(x, 7, 0), pltpu.roll(x, 1, 0)
                eu_, ed_ = pltpu.roll(ee, 7, 0), pltpu.roll(ee, 1, 0)
                b = jnp.where(sub == 7, eu_, xu) - jnp.where(sub == 0, ed_, xd)
                hs[l, d] = jnp.where(sub == 0, eu_ - xd, xu - ed_)
                bs[l, d] = b
                z.append((x, b))
            store_spec(l, dft16(z))
        store_spec(2, dft16([(hs[0, d], hs[1, d]) for d in range(16)]))
        spec = big_dot(lhs[...])
        for t, f in ((0, fo), (1, fo), (2, fh)):
            lhs[t * 128 : t * 128 + 128, 0:128] = spec[t * 128 : t * 128 + 128, 128:256] * f[...]
            lhs[t * 128 : t * 128 + 128, 128:256] = spec[t * 128 : t * 128 + 128, 0:128] * f[...]
        res[...] = big_dot(lhs[...])
        hh = unfold(2)
        for d in range(16):
            for l in range(2):
                hs[l, d] = -mch * jnp.where(keep_h, hh[d][l], hs[l, d])
        for l in range(2):
            y = unfold(l)
            fa = [jnp.where(keep_o, y[d][0], get_main(ph, d, l)) for d in range(16)]
            for d in range(16):
                dvd = -mc * jnp.where(keep_o, y[d][1], bs[l, d])
                hv = hs[l, d]
                north = pltpu.roll(jnp.where(sub == 0, hv, dvd), 7, 0)
                south = pltpu.roll(jnp.where(sub == 7, hv, dvd), 1, 0)
                nx, pv_ = fa[(d + 1) % 16], fa[(d + 15) % 16]
                r2 = pltpu.roll(jnp.where(lane < 2, nx, fa[d]), 126, 1)
                l2 = pltpu.roll(jnp.where(lane >= 126, pv_, fa[d]), 2, 1)
                dd = (r2 - fa[d]) - (fa[d] - l2)
                dsend[ph, d, l] = mc * (north - south) - zc * zc * dd
                if ph == SUBSTEPS - 1:
                    dv[d, l] = dvd
                    r1 = pltpu.roll(jnp.where(lane < 1, nx, fa[d]), 127, 1)
                    l1 = pltpu.roll(jnp.where(lane >= 127, pv_, fa[d]), 1, 1)
                    du[d, l] = -zc * (r1 - l1)

    def backward(src, dst, si, sem):
        for off in OFFS:
            d = target(off)
            if off != (0, 0):
                rcopy(src.at[d], dst.at[pl.ds(2 * me, 2)], si, sem, g, d)
        dst[pl.ds(2 * me, 2)] = src[pl.ds(me, 1)][0]

    def wait30(buf, sem):
        pltpu.make_async_copy(buf.at[pl.ds(0, 30)], buf.at[pl.ds(0, 30)], sem).wait()

    def column(ph, pin, win, pout, wout):
        ps = [pin[k] - sv[k] * (div0[k] + back[ph, k]) for k in range(NL)]
        vals = []
        pval = jnp.zeros((8, 128), F32)
        for k in range(NL):
            al = a_s[k]
            if k + 1 < NL:
                rhs = win[k] - al * (ps[k + 1] - ps[k])
            else:
                rhs = win[k] + al * ps[k]
            pval = rhs * inv[k] + qq[k] * pval
            vals.append(pval)
        wk = vals[-1]
        for k in range(NL - 1, -1, -1):
            wout[k] = wk
            if k:
                wlow = vals[k - 1] - rat[k - 1] * wk
                pout[k] = ps[k] - sv[k] * (wk - wlow)
                wk = wlow
            else:
                pout[k] = ps[k] - sv[k] * wk

    outs = []

    def put(src, dst, i):
        c = pltpu.make_async_copy(src, dst, outsem.at[i])
        c.start()
        outs.append(c)

    level_part(0)
    backward(dsend.at[0], back.at[0], 10, bksem.at[0])
    wait30(back.at[0], bksem.at[0])
    column(0, pv, wv, p1, w1)
    forward(1, p1)
    level_part(1)
    backward(dsend.at[1], back.at[1], 11, bksem.at[1])
    backward(du, ru, 12, bksem.at[2])
    backward(dv, rv, 13, bksem.at[3])
    wait30(back.at[1], bksem.at[1])
    column(1, p1, w1, p2, w2)
    put(w2, wo_h, 0)
    put(p2, po_h, 1)
    wait30(ru, bksem.at[2])
    for k in range(NL):
        ru[k] = ru[k] + uv[k]
    put(ru, uo_h, 2)
    wait30(rv, bksem.at[3])
    for k in range(NL):
        rv[k] = rv[k] + vv[k]
    put(rv, vo_h, 3)

    for ph in range(SUBSTEPS):
        wait15(xm.at[ph], sendsem.at[3 * ph])
        wait_all(xe.at[ph, :, :, 0:2], sendsem.at[3 * ph + 1])
        wait_all(xe.at[ph, :, :, 0:2], sendsem.at[3 * ph + 2])
    wait_all(back.at[0, 0:2], sendsem.at[6])
    wait_all(back.at[0, 0:2], sendsem.at[7])
    wait_all(ev.at[:, 0:1], sendsem.at[8])
    wait_all(ev.at[:, 0:1], sendsem.at[9])
    for i in range(10, 14):
        wait30(ru, sendsem.at[i])
    for c in outs:
        c.wait()


def solution(mesh):
    mat_np, tw_np = tables()
    field = jax.ShapeDtypeStruct((NL, 8, 128), F32)
    smem = pl.BlockSpec(memory_space=pltpu.SMEM)
    hbm = pl.BlockSpec(memory_space=pltpu.HBM)
    blk = pltpu.VMEM((NL, 8, 128), F32)
    pair = pltpu.VMEM((2, 16, 8, 128), F32)
    quad = pltpu.VMEM((2, 16, 2, 8, 128), F32)
    line = pltpu.VMEM((8, 128), F32)
    rows = pltpu.VMEM((384, 256), F32)
    dma = pltpu.SemaphoreType.DMA
    scratch = [
        blk, blk, blk, blk, blk, pltpu.VMEM((256, 256), F32), pltpu.VMEM((2, 16, 128), F32),
        blk, blk, blk, blk, quad, quad, pair, pair, rows, rows, quad, pltpu.VMEM((2, NL, 8, 128), F32),
        pltpu.VMEM((16, 2, 8, 128), F32), pltpu.VMEM((16, 2, 8, 128), F32), blk, blk,
        blk, blk, blk, blk, line, line, line, blk, line, line, line,
        pltpu.VMEM((128, 128), F32), pltpu.VMEM((128, 128), F32),
        dma((7,)), dma((4,)), dma((14,)), dma((2,)), dma((2, 2)), dma((4,)), dma((6,)),
    ]
    call = pl.pallas_call(
        kernel,
        out_shape=(field,) * 4,
        in_specs=[smem] * 5 + [hbm] * 7,
        out_specs=(hbm,) * 4,
        scratch_shapes=scratch,
        compiler_params=pltpu.CompilerParams(collective_id=0, has_side_effects=True),
    )

    def body(u, v, w, p, zc, mc, a, s, cutoff, mask):
        return call(zc, mc, a, cutoff, mask, u, v, w, p, s, jnp.asarray(mat_np), jnp.asarray(tw_np))

    f = P(None, "lat", "lon")
    return jax.shard_map(
        body,
        mesh=mesh,
        in_specs=(f, f, f, f, P("lat"), P("lat"), P(None), f, P(None), P(None)),
        out_specs=(f,) * 4,
        check_vma=False,
    )
```

```python
import math

import jax
import jax.numpy as jnp
import numpy as np
from jax import lax
from jax.experimental import pallas as pl
from jax.experimental.pallas import tpu as pltpu
from jax.sharding import PartitionSpec as P

SUBSTEPS = 2
F32 = jnp.float32
NG = 8
ND = 16
NL = 32
MESH = pl.DeviceIdType.MESH


def tables():
    lane = np.arange(128)
    ang = 2.0 * np.pi * ((lane[:, None] * lane[None, :]) % 128) / 128.0
    c, s = np.cos(ang), np.sin(ang)
    mat = np.block([[c, -s], [s, c]])
    high = mat.astype(np.float32).astype(jnp.bfloat16)
    low = (mat - high.astype(np.float64)).astype(np.float32).astype(jnp.bfloat16)
    mat = np.stack([high, low])
    tang = 2.0 * np.pi * (np.arange(16)[:, None] * lane[None, :]) / 2048.0
    tw = np.stack([np.cos(tang), -np.sin(tang)]).astype(np.float32)
    return mat, tw


def dft4(x):
    (ar, ai), (br, bi), (cr, ci), (dr, di) = x
    sr, si = ar + cr, ai + ci
    tr, ti = ar - cr, ai - ci
    ur, ui = br + dr, bi + di
    vr, vi = br - dr, bi - di
    return [(sr + ur, si + ui), (tr + vi, ti - vr), (sr - ur, si - ui), (tr - vi, ti + vr)]


def dft16(x):
    cols = []
    for n2 in range(4):
        y = dft4([x[4 * n1 + n2] for n1 in range(4)])
        out = []
        for k1 in range(4):
            e = (n2 * k1) % 16
            yr, yi = y[k1]
            if e == 0:
                out.append((yr, yi))
            elif e == 4:
                out.append((yi, -yr))
            else:
                c, s = math.cos(2 * math.pi * e / 16), math.sin(2 * math.pi * e / 16)
                out.append((yr * c + yi * s, yi * c - yr * s))
        cols.append(out)
    res = [None] * 16
    for k1 in range(4):
        z = dft4([cols[n2][k1] for n2 in range(4)])
        for k2 in range(4):
            res[k1 + 4 * k2] = z[k2]
    return res


def hops(off):
    return sum(min(o, 4 - o) for o in off)


OFFS = sorted([(a, b) for a in range(4) for b in range(4)], key=lambda o: -hops(o))


def kernel(
    zc_h, mc_h, a_h, cut_h, msk_h, u_h, v_h, w_h, p_h, s_h, mat_h, tw_h,
    uo, vo, w2, p2,
    uv, vv, wv, pv, sv, mat, tw, p1, w1, xm, xe, bs, hs, lhs, res, dsend, back,
    du, dv, ru, rv, rat, inv, qq, div0, eu, eul, eur, ev, mct, mcp, mcn, fo, fh,
    zc_s, mc_s, a_s, cut_s, msk_s,
    ldsem, smsem, sendsem, fmsem, fesem, bksem, esem,
):
    me = lax.axis_index("lon")
    g = lax.axis_index("lat")
    up = (g + 1) % NG
    dn = (g + NG - 1) % NG
    my, mx = me // 4, me % 4
    east = (me + 1) % ND
    west = (me + ND - 1) % ND

    loads = [
        pltpu.make_async_copy(a, b, ldsem.at[i])
        for i, (a, b) in enumerate(
            [(p_h, pv), (u_h, uv), (v_h, vv), (s_h, sv), (w_h, wv), (tw_h, tw), (mat_h, mat)]
        )
    ]
    small = [
        pltpu.make_async_copy(a, b, smsem.at[i])
        for i, (a, b) in enumerate(
            [(zc_h, zc_s), (mc_h, mc_s), (a_h, a_s), (cut_h, cut_s), (msk_h, msk_s)]
        )
    ]
    bar = pltpu.get_barrier_semaphore()

    def target(off):
        return ((my + off[0]) % 4) * 4 + (mx + off[1]) % 4

    for off in OFFS:
        d = target(off)
        pl.semaphore_signal(bar, inc=1, device_id={"lat": up, "lon": d}, device_id_type=MESH)
        pl.semaphore_signal(bar, inc=1, device_id={"lat": dn, "lon": d}, device_id_type=MESH)
        if off != (0, 0):
            pl.semaphore_signal(bar, inc=1, device_id={"lat": g, "lon": d}, device_id_type=MESH)

    for c in loads[:1] + small + loads[1:]:
        c.start()

    def rcopy(src, dst, si, sem, gg, d):
        c = pltpu.make_async_remote_copy(
            src_ref=src, dst_ref=dst, send_sem=sendsem.at[si], recv_sem=sem,
            device_id={"lat": gg, "lon": d}, device_id_type=MESH,
        )
        c.start()

    def forward(ph, src):
        for off in OFFS:
            d = target(off)
            if off != (0, 0):
                rcopy(src.at[pl.ds(2 * d, 2)], xm.at[ph, me], 3 * ph, fmsem.at[ph], g, d)
            rcopy(src.at[pl.ds(2 * d, 2), 6:8], xe.at[ph, me, :, 6:8], 3 * ph + 1, fesem.at[ph, 0], up, d)
            rcopy(src.at[pl.ds(2 * d, 2), 0:2], xe.at[ph, me, :, 0:2], 3 * ph + 2, fesem.at[ph, 1], dn, d)
        xm[ph, pl.ds(me, 1)] = src[pl.ds(2 * me, 2)][None]

    def wait15(buf, sem):
        pltpu.make_async_copy(buf.at[pl.ds(0, 15)], buf.at[pl.ds(0, 15)], sem).wait()

    def wait_all(buf, sem):
        pltpu.make_async_copy(buf, buf, sem).wait()

    sub = lax.broadcasted_iota(jnp.int32, (8, 128), 0)
    lane = lax.broadcasted_iota(jnp.int32, (8, 128), 1)

    def tile(read):
        t = jnp.full((8, 128), read(0))
        for r in range(1, 8):
            t = jnp.where(sub == r, read(r), t)
        return t

    valid = jnp.logical_or(
        jnp.logical_and(sub >= 4, jnp.full((8, 128), g) > 0),
        jnp.logical_and(sub < 4, jnp.full((8, 128), g) < NG - 1),
    )

    with jax.named_scope("entry"):
        loads[0].wait()
        pl.semaphore_wait(bar, 47)
    with jax.named_scope("fwd0"):
        forward(0, pv)
        for c in small:
            c.wait()
        zc = tile(lambda r: zc_s[r])
        mc = tile(lambda r: mc_s[r])
        mct[...] = mc
        own = lambda ref: tile(lambda r: ref[8 * g + r])
        halo = lambda ref: jnp.where(sub == 0, ref[(8 * g + 8) % 64], ref[(8 * g + 63) % 64])
        keep_o = own(msk_s) > 0
        keep_h = halo(msk_s) > 0
        rcopy(mct, mcp, 6, esem.at[0], up, me)
        rcopy(mct, mcn, 6, esem.at[1], dn, me)
    with jax.named_scope("home"):
        loads[1].wait()
        e = jnp.zeros((8, 128), F32)
        for k in range(NL):
            uk = uv[k]
            e = jnp.where(lane == k, pltpu.roll(uk, (k + 1) % 128, 1), e)
            e = jnp.where(lane == 32 + k, pltpu.roll(uk, 32 + k, 1), e)
        eu[...] = e
        rcopy(eu, eul, 7, esem.at[2], g, east)
        rcopy(eu, eur, 7, esem.at[3], g, west)
        loads[2].wait()
        rcopy(vv.at[:, 7:8], ev.at[:, 7:8], 8, esem.at[4], up, me)
        rcopy(vv.at[:, 0:1], ev.at[:, 0:1], 9, esem.at[5], dn, me)

        def factors(cut):
            k1 = lax.broadcasted_iota(jnp.int32, (16, 8, 128), 0)
            k2 = lax.broadcasted_iota(jnp.int32, (16, 8, 128), 2)
            k = k1 + 16 * k2
            kk = jnp.minimum(k, 2048 - k).astype(F32)
            c = cut.astype(F32)[None]
            ratio = c / jnp.maximum(kk, 1.0)
            f = jnp.where(kk > c, ratio * ratio, 1.0) * (1.0 / 2048.0)
            return f.reshape(128, 128)

        fo[...] = factors(own(cut_s))
        fh[...] = factors(halo(cut_s))

        loads[3].wait()
        prev = jnp.zeros((8, 128), F32)
        for k in range(NL):
            al = a_s[k]
            below = al * sv[k]
            above = al * sv[k + 1] if k + 1 < NL else jnp.zeros((8, 128), F32)
            ip = 1.0 / (1.0 + below + above + below * prev)
            prev = -above * ip
            rat[k] = prev
            inv[k] = ip
            qq[k] = below * ip

        wait_all(mcp, esem.at[0])
        wait_all(mcn, esem.at[1])
        mch = jnp.where(sub >= 4, mcp[...], mcn[...])
        mch = jnp.where(valid, mch, 0.0)
        wait_all(eul, esem.at[2])
        wait_all(eur, esem.at[3])
        wait_all(ev.at[:, 7:8], esem.at[4])
        wait_all(ev.at[:, 0:1], esem.at[5])
        el, er = eul[...], eur[...]
        for k in range(NL):
            uk, vk = uv[k], vv[k]
            evk = jnp.where(valid, ev[k], 0.0)
            right = jnp.where(lane == 127, pltpu.roll(er, (95 - k) % 128, 1), pltpu.roll(uk, 127, 1))
            left = jnp.where(lane == 0, pltpu.roll(el, (128 - k) % 128, 1), pltpu.roll(uk, 1, 1))
            north = pltpu.roll(jnp.where(sub == 0, evk, vk), 7, 0)
            south = pltpu.roll(jnp.where(sub == 7, evk, vk), 1, 0)
            div0[k] = zc * (right - left) + mc * (north - south)
    loads[4].wait()
    loads[5].wait()
    loads[6].wait()

    def get_main(ph, d, l):
        x = xm[0, d, l]
        return x + xm[1, d, l] if ph else x

    def get_edge(ph, d, l):
        x = xe[0, d, l]
        x = x + xe[1, d, l] if ph else x
        return jnp.where(valid, x, 0.0)

    def store_spec(t, spec):
        for k1 in range(16):
            r, i = spec[k1]
            tr, ti = tw[0, k1 : k1 + 1, :], tw[1, k1 : k1 + 1, :]
            row = t * 128 + k1 * 8
            lhs[row : row + 8, 0:128] = r * tr - i * ti
            lhs[row : row + 8, 128:256] = r * ti + i * tr

    def big_dot(x):
        high = x.astype(jnp.bfloat16)
        low = (x - high.astype(F32)).astype(jnp.bfloat16)
        one = lambda a, b: jnp.dot(a, b, preferred_element_type=F32)
        return one(high, mat[0]) + one(low, mat[0]) + one(high, mat[1])

    def unfold(t):
        x = []
        for k1 in range(16):
            row = t * 128 + k1 * 8
            r, i = res[row : row + 8, 0:128], res[row : row + 8, 128:256]
            tr, ti = tw[0, k1 : k1 + 1, :], tw[1, k1 : k1 + 1, :]
            x.append((r * tr - i * ti, r * ti + i * tr))
        return [(b, a) for a, b in dft16(x)]

    def level_part(ph):
        with jax.named_scope("waitf%d" % ph):
            wait15(xm.at[ph], fmsem.at[ph])
            wait_all(xe.at[ph, :, :, 0:2], fesem.at[ph, 0])
            wait_all(xe.at[ph, :, :, 0:2], fesem.at[ph, 1])
        with jax.named_scope("fold%d" % ph):
            for l in range(2):
                z = []
                for d in range(16):
                    x, ee = get_main(ph, d, l), get_edge(ph, d, l)
                    xu, xd = pltpu.roll(x, 7, 0), pltpu.roll(x, 1, 0)
                    eu_, ed_ = pltpu.roll(ee, 7, 0), pltpu.roll(ee, 1, 0)
                    b = jnp.where(sub == 7, eu_, xu) - jnp.where(sub == 0, ed_, xd)
                    hs[l, d] = jnp.where(sub == 0, eu_ - xd, xu - ed_)
                    bs[l, d] = b
                    z.append((x, b))
                store_spec(l, dft16(z))
            store_spec(2, dft16([(hs[0, d], hs[1, d]) for d in range(16)]))
        with jax.named_scope("dots%d" % ph):
            spec = big_dot(lhs[...])
            for t, f in ((0, fo), (1, fo), (2, fh)):
                lhs[t * 128 : t * 128 + 128, 0:128] = spec[t * 128 : t * 128 + 128, 128:256] * f[...]
                lhs[t * 128 : t * 128 + 128, 128:256] = spec[t * 128 : t * 128 + 128, 0:128] * f[...]
            res[...] = big_dot(lhs[...])
        with jax.named_scope("unfold%d" % ph):
            hh = unfold(2)
            for d in range(16):
                for l in range(2):
                    hs[l, d] = -mch * jnp.where(keep_h, hh[d][l], hs[l, d])
            for l in range(2):
                y = unfold(l)
                fa = [jnp.where(keep_o, y[d][0], get_main(ph, d, l)) for d in range(16)]
                for d in range(16):
                    dvd = -mc * jnp.where(keep_o, y[d][1], bs[l, d])
                    hv = hs[l, d]
                    north = pltpu.roll(jnp.where(sub == 0, hv, dvd), 7, 0)
                    south = pltpu.roll(jnp.where(sub == 7, hv, dvd), 1, 0)
                    nx, pv_ = fa[(d + 1) % 16], fa[(d + 15) % 16]
                    r2 = pltpu.roll(jnp.where(lane < 2, nx, fa[d]), 126, 1)
                    l2 = pltpu.roll(jnp.where(lane >= 126, pv_, fa[d]), 2, 1)
                    dd = (r2 - fa[d]) - (fa[d] - l2)
                    dsend[ph, d, l] = mc * (north - south) - zc * zc * dd
                    if ph == SUBSTEPS - 1:
                        dv[d, l] = dvd
                        r1 = pltpu.roll(jnp.where(lane < 1, nx, fa[d]), 127, 1)
                        l1 = pltpu.roll(jnp.where(lane >= 127, pv_, fa[d]), 1, 1)
                        du[d, l] = -zc * (r1 - l1)
    def backward(src, dst, si, sem):
        for off in OFFS:
            d = target(off)
            if off != (0, 0):
                rcopy(src.at[d], dst.at[pl.ds(2 * me, 2)], si, sem, g, d)
        dst[pl.ds(2 * me, 2)] = src[pl.ds(me, 1)][0]

    def wait30(buf, sem):
        pltpu.make_async_copy(buf.at[pl.ds(0, 30)], buf.at[pl.ds(0, 30)], sem).wait()

    def column(ph, pin, win, pout, wout):
        ps = [pin[k] - sv[k] * (div0[k] + back[ph, k]) for k in range(NL)]
        vals = []
        pval = jnp.zeros((8, 128), F32)
        for k in range(NL):
            al = a_s[k]
            if k + 1 < NL:
                rhs = win[k] - al * (ps[k + 1] - ps[k])
            else:
                rhs = win[k] + al * ps[k]
            pval = rhs * inv[k] + qq[k] * pval
            vals.append(pval)
        wk = vals[-1]
        for k in range(NL - 1, -1, -1):
            wout[k] = wk
            if k:
                wlow = vals[k - 1] - rat[k - 1] * wk
                pout[k] = ps[k] - sv[k] * (wk - wlow)
                wk = wlow
            else:
                pout[k] = ps[k] - sv[k] * wk

    level_part(0)
    with jax.named_scope("bk0"):
        backward(dsend.at[0], back.at[0], 10, bksem.at[0])
    with jax.named_scope("waitb0"):
        wait30(back.at[0], bksem.at[0])
    with jax.named_scope("col0"):
        column(0, pv, wv, p1, w1)
    with jax.named_scope("fwd1"):
        forward(1, p1)
    level_part(1)
    with jax.named_scope("bk1"):
        backward(dsend.at[1], back.at[1], 11, bksem.at[1])
        backward(du, ru, 12, bksem.at[2])
        backward(dv, rv, 13, bksem.at[3])
    with jax.named_scope("waitb1"):
        wait30(back.at[1], bksem.at[1])
    with jax.named_scope("col1"):
        column(1, p1, w1, p2, w2)
    with jax.named_scope("fin"):
        wait30(ru, bksem.at[2])
        for k in range(NL):
            uo[k] = ru[k] + uv[k]
        wait30(rv, bksem.at[3])
        for k in range(NL):
            vo[k] = rv[k] + vv[k]
    with jax.named_scope("sends"):
        for ph in range(SUBSTEPS):
            wait15(xm.at[ph], sendsem.at[3 * ph])
            wait_all(xe.at[ph, :, :, 0:2], sendsem.at[3 * ph + 1])
            wait_all(xe.at[ph, :, :, 0:2], sendsem.at[3 * ph + 2])
        wait_all(back.at[0, 0:2], sendsem.at[6])
        wait_all(back.at[0, 0:2], sendsem.at[7])
        wait_all(ev.at[:, 0:1], sendsem.at[8])
        wait_all(ev.at[:, 0:1], sendsem.at[9])
        for i in range(10, 14):
            wait30(ru, sendsem.at[i])

def store(u, v, w, p, uo, vo, wo, po, sem):
    copies = [pltpu.make_async_copy(a, b, sem.at[i]) for i, (a, b) in enumerate([(u, uo), (v, vo), (w, wo), (p, po)])]
    for c in copies:
        c.start()
    for c in copies:
        c.wait()


def solution(mesh):
    mat_np, tw_np = tables()
    field = jax.ShapeDtypeStruct((NL, 8, 128), F32)
    vmem = pl.BlockSpec(memory_space=pltpu.VMEM)
    hbm = pl.BlockSpec(memory_space=pltpu.HBM)
    blk = pltpu.VMEM((NL, 8, 128), F32)
    pair = pltpu.VMEM((2, 16, 8, 128), F32)
    quad = pltpu.VMEM((2, 16, 2, 8, 128), F32)
    line = pltpu.VMEM((8, 128), F32)
    rows = pltpu.VMEM((384, 256), F32)
    dma = pltpu.SemaphoreType.DMA
    scratch = [
        blk, blk, blk, blk, blk, pltpu.VMEM((2, 256, 256), jnp.bfloat16), pltpu.VMEM((2, 16, 128), F32),
        blk, blk, quad, quad, pair, pair, rows, rows, quad, pltpu.VMEM((2, NL, 8, 128), F32),
        pltpu.VMEM((16, 2, 8, 128), F32), pltpu.VMEM((16, 2, 8, 128), F32), blk, blk,
        blk, blk, blk, blk, line, line, line, blk, line, line, line,
        pltpu.VMEM((128, 128), F32), pltpu.VMEM((128, 128), F32),
        pltpu.SMEM((8,), F32), pltpu.SMEM((8,), F32), pltpu.SMEM((NL,), F32), pltpu.SMEM((64,), jnp.int32), pltpu.SMEM((64,), jnp.int32),
        dma((7,)), dma((5,)), dma((14,)), dma((2,)), dma((2, 2)), dma((4,)), dma((6,)),
    ]
    call = pl.pallas_call(
        kernel,
        out_shape=(blk,) * 4,
        in_specs=[hbm] * 12,
        out_specs=(vmem,) * 4,
        scratch_shapes=scratch,
        compiler_params=pltpu.CompilerParams(collective_id=0, has_side_effects=True),
    )

    finish = pl.pallas_call(
        store, out_shape=(field,) * 4, in_specs=[vmem] * 4, out_specs=(hbm,) * 4, scratch_shapes=[dma((4,))]
    )

    def hold(*xs):
        return [pltpu.with_memory_space_constraint(o, pltpu.VMEM) for o in call(*xs)]

    def body(u, v, w, p, zc, mc, a, s, cutoff, mask):
        return finish(*hold(zc, mc, a, cutoff, mask, u, v, w, p, s, jnp.asarray(mat_np), jnp.asarray(tw_np)))

    f = P(None, "lat", "lon")
    return jax.shard_map(
        body,
        mesh=mesh,
        in_specs=(f, f, f, f, P("lat"), P("lat"), P(None), f, P(None), P(None)),
        out_specs=(f,) * 4,
        check_vma=False,
    )
```

```python
import math

import jax
import jax.numpy as jnp
import numpy as np
from jax import lax
from jax.experimental import pallas as pl
from jax.experimental.pallas import tpu as pltpu
from jax.sharding import PartitionSpec as P

SUBSTEPS = 2
F32 = jnp.float32
NG = 8
ND = 16
NL = 32
MESH = pl.DeviceIdType.MESH


def tables():
    lane = np.arange(128)
    ang = 2.0 * np.pi * ((lane[:, None] * lane[None, :]) % 128) / 128.0
    c, s = np.cos(ang), np.sin(ang)
    mat = np.block([[c, -s], [s, c]])
    high = mat.astype(np.float32).astype(jnp.bfloat16)
    low = (mat - high.astype(np.float64)).astype(np.float32).astype(jnp.bfloat16)
    mat = np.concatenate([high, high, low])
    tang = 2.0 * np.pi * (np.arange(16)[:, None] * lane[None, :]) / 2048.0
    tw = np.stack([np.cos(tang), -np.sin(tang)]).astype(np.float32)
    return mat, tw


def dft4(x):
    (ar, ai), (br, bi), (cr, ci), (dr, di) = x
    sr, si = ar + cr, ai + ci
    tr, ti = ar - cr, ai - ci
    ur, ui = br + dr, bi + di
    vr, vi = br - dr, bi - di
    return [(sr + ur, si + ui), (tr + vi, ti - vr), (sr - ur, si - ui), (tr - vi, ti + vr)]


def dft16(x):
    cols = []
    for n2 in range(4):
        y = dft4([x[4 * n1 + n2] for n1 in range(4)])
        out = []
        for k1 in range(4):
            e = (n2 * k1) % 16
            yr, yi = y[k1]
            if e == 0:
                out.append((yr, yi))
            elif e == 4:
                out.append((yi, -yr))
            else:
                c, s = math.cos(2 * math.pi * e / 16), math.sin(2 * math.pi * e / 16)
                out.append((yr * c + yi * s, yi * c - yr * s))
        cols.append(out)
    res = [None] * 16
    for k1 in range(4):
        z = dft4([cols[n2][k1] for n2 in range(4)])
        for k2 in range(4):
            res[k1 + 4 * k2] = z[k2]
    return res


def hops(off):
    return sum(min(o, 4 - o) for o in off)


OFFS = sorted([(a, b) for a in range(4) for b in range(4)], key=lambda o: -hops(o))


def kernel(
    zc_h, mc_h, a_h, cut_h, msk_h, u_h, v_h, w_h, p_h, s_h, mat_h, tw_h,
    uo, vo, w2, p2,
    uv, vv, wv, pv, sv, mat, tw, p1, w1, xm, xe, lhs, res, dsend, back,
    du, dv, ru, rv, rat, inv, qq, div0, eu, eul, eur, ev, mct, mcp, mcn, fo, fb, fh,
    zc_s, mc_s, a_s, cut_s, msk_s,
    ldsem, smsem, sendsem, fmsem, fesem, bksem, esem,
):
    me = lax.axis_index("lon")
    g = lax.axis_index("lat")
    up = (g + 1) % NG
    dn = (g + NG - 1) % NG
    my, mx = me // 4, me % 4
    east = (me + 1) % ND
    west = (me + ND - 1) % ND

    loads = [
        pltpu.make_async_copy(a, b, ldsem.at[i])
        for i, (a, b) in enumerate(
            [(p_h, pv), (u_h, uv), (v_h, vv), (s_h, sv), (w_h, wv), (tw_h, tw), (mat_h, mat)]
        )
    ]
    small = [
        pltpu.make_async_copy(a, b, smsem.at[i])
        for i, (a, b) in enumerate(
            [(zc_h, zc_s), (mc_h, mc_s), (a_h, a_s), (cut_h, cut_s), (msk_h, msk_s)]
        )
    ]
    bar = pltpu.get_barrier_semaphore()

    def target(off):
        return ((my + off[0]) % 4) * 4 + (mx + off[1]) % 4

    for off in OFFS:
        d = target(off)
        pl.semaphore_signal(bar, inc=1, device_id={"lat": up, "lon": d}, device_id_type=MESH)
        pl.semaphore_signal(bar, inc=1, device_id={"lat": dn, "lon": d}, device_id_type=MESH)
        if off != (0, 0):
            pl.semaphore_signal(bar, inc=1, device_id={"lat": g, "lon": d}, device_id_type=MESH)

    for c in loads[:1] + small + loads[1:]:
        c.start()

    def rcopy(src, dst, si, sem, gg, d):
        c = pltpu.make_async_remote_copy(
            src_ref=src, dst_ref=dst, send_sem=sendsem.at[si], recv_sem=sem,
            device_id={"lat": gg, "lon": d}, device_id_type=MESH,
        )
        c.start()

    def forward(ph, src):
        for off in OFFS:
            d = target(off)
            rcopy(src.at[pl.ds(2 * d, 2), 6:8], xe.at[ph, me, :, 6:8], 3 * ph + 1, fesem.at[ph, 0], up, d)
            rcopy(src.at[pl.ds(2 * d, 2), 0:2], xe.at[ph, me, :, 0:2], 3 * ph + 2, fesem.at[ph, 1], dn, d)
        for off in OFFS:
            d = target(off)
            if off != (0, 0):
                rcopy(src.at[pl.ds(2 * d, 2)], xm.at[ph, me], 3 * ph, fmsem.at[ph], g, d)
        xm[ph, pl.ds(me, 1)] = src[pl.ds(2 * me, 2)][None]

    def wait15(buf, sem):
        pltpu.make_async_copy(buf.at[pl.ds(0, 15)], buf.at[pl.ds(0, 15)], sem).wait()

    def wait_all(buf, sem):
        pltpu.make_async_copy(buf, buf, sem).wait()

    sub = lax.broadcasted_iota(jnp.int32, (8, 128), 0)
    lane = lax.broadcasted_iota(jnp.int32, (8, 128), 1)

    def tile(read):
        t = jnp.full((8, 128), read(0))
        for r in range(1, 8):
            t = jnp.where(sub == r, read(r), t)
        return t

    valid = jnp.logical_or(
        jnp.logical_and(sub >= 4, jnp.full((8, 128), g) > 0),
        jnp.logical_and(sub < 4, jnp.full((8, 128), g) < NG - 1),
    )

    with jax.named_scope("entry"):
        loads[0].wait()
        pl.semaphore_wait(bar, 47)
    with jax.named_scope("fwd0"):
        forward(0, pv)
        for c in small:
            c.wait()
        zc = tile(lambda r: zc_s[r])
        mc = tile(lambda r: mc_s[r])
        mct[...] = mc
        own = lambda ref: tile(lambda r: ref[8 * g + r])
        halo = lambda ref: jnp.where(sub == 0, ref[(8 * g + 8) % 64], ref[(8 * g + 63) % 64])
        rcopy(mct, mcp, 6, esem.at[0], up, me)
        rcopy(mct, mcn, 6, esem.at[1], dn, me)
    with jax.named_scope("home"):
        loads[1].wait()
        e = jnp.zeros((8, 128), F32)
        for k in range(NL):
            uk = uv[k]
            e = jnp.where(lane == k, pltpu.roll(uk, (k + 1) % 128, 1), e)
            e = jnp.where(lane == 32 + k, pltpu.roll(uk, 32 + k, 1), e)
        eu[...] = e
        rcopy(eu, eul, 7, esem.at[2], g, east)
        rcopy(eu, eur, 7, esem.at[3], g, west)
        loads[2].wait()
        rcopy(vv.at[:, 7:8], ev.at[:, 7:8], 8, esem.at[4], up, me)
        rcopy(vv.at[:, 0:1], ev.at[:, 0:1], 9, esem.at[5], dn, me)

        def factors(cut, mask):
            k1 = lax.broadcasted_iota(jnp.int32, (16, 8, 128), 0)
            k2 = lax.broadcasted_iota(jnp.int32, (16, 8, 128), 2)
            k = k1 + 16 * k2
            kk = jnp.minimum(k, 2048 - k).astype(F32)
            c = cut.astype(F32)[None]
            ratio = c / jnp.maximum(kk, 1.0)
            damped = jnp.logical_and(kk > c, mask[None] > 0)
            return jnp.where(damped, ratio * ratio, 1.0) * (1.0 / 2048.0)

        fo[...] = factors(own(cut_s), own(msk_s)).reshape(128, 128)
        fb[...] = (-mc[None] * factors(own(cut_s), own(msk_s))).reshape(128, 128)

        loads[3].wait()
        prev = jnp.zeros((8, 128), F32)
        for k in range(NL):
            al = a_s[k]
            below = al * sv[k]
            above = al * sv[k + 1] if k + 1 < NL else jnp.zeros((8, 128), F32)
            ip = 1.0 / (1.0 + below + above + below * prev)
            prev = -above * ip
            rat[k] = prev
            inv[k] = ip
            qq[k] = below * ip

        wait_all(mcp, esem.at[0])
        wait_all(mcn, esem.at[1])
        mch = jnp.where(sub >= 4, mcp[...], mcn[...])
        mch = jnp.where(valid, mch, 0.0)
        fh[...] = (-mch[None] * factors(halo(cut_s), halo(msk_s))).reshape(128, 128)
        wait_all(eul, esem.at[2])
        wait_all(eur, esem.at[3])
        wait_all(ev.at[:, 7:8], esem.at[4])
        wait_all(ev.at[:, 0:1], esem.at[5])
        el, er = eul[...], eur[...]
        for k in range(NL):
            uk, vk = uv[k], vv[k]
            evk = jnp.where(valid, ev[k], 0.0)
            right = jnp.where(lane == 127, pltpu.roll(er, (95 - k) % 128, 1), pltpu.roll(uk, 127, 1))
            left = jnp.where(lane == 0, pltpu.roll(el, (128 - k) % 128, 1), pltpu.roll(uk, 1, 1))
            north = pltpu.roll(jnp.where(sub == 0, evk, vk), 7, 0)
            south = pltpu.roll(jnp.where(sub == 7, evk, vk), 1, 0)
            div0[k] = zc * (right - left) + mc * (north - south)
    loads[4].wait()
    loads[5].wait()
    loads[6].wait()

    def get_main(ph, d, l):
        x = xm[0, d, l]
        return x + xm[1, d, l] if ph else x

    def get_edge(ph, d, l):
        x = xe[0, d, l]
        x = x + xe[1, d, l] if ph else x
        return jnp.where(valid, x, 0.0)

    def store_spec(t, spec):
        for k1 in range(16):
            r, i = spec[k1]
            tr, ti = tw[0, k1 : k1 + 1, :], tw[1, k1 : k1 + 1, :]
            row = t * 128 + k1 * 8
            lhs[row : row + 8, 0:128] = r * tr - i * ti
            lhs[row : row + 8, 128:256] = r * ti + i * tr

    def big_dot(x):
        high = x.astype(jnp.bfloat16)
        low = (x - high.astype(F32)).astype(jnp.bfloat16)
        one = lambda a, b: jnp.dot(a, b, preferred_element_type=F32)
        return one(jnp.concatenate([high, low, high], axis=1), mat[...])

    def unfold(t):
        x = []
        for k1 in range(16):
            row = t * 128 + k1 * 8
            r, i = res[row : row + 8, 0:128], res[row : row + 8, 128:256]
            tr, ti = tw[0, k1 : k1 + 1, :], tw[1, k1 : k1 + 1, :]
            x.append((r * tr - i * ti, r * ti + i * tr))
        return [(b, a) for a, b in dft16(x)]

    def backward(src, dst, si, sem):
        for off in OFFS:
            d = target(off)
            if off != (0, 0):
                rcopy(src.at[d], dst.at[pl.ds(2 * me, 2)], si, sem, g, d)
        dst[pl.ds(2 * me, 2)] = src[pl.ds(me, 1)][0]

    def wait30(buf, sem):
        pltpu.make_async_copy(buf.at[pl.ds(0, 30)], buf.at[pl.ds(0, 30)], sem).wait()

    def filtered(t, spec, f):
        turned = jnp.concatenate([spec[:, 128:256] * f[...], spec[:, 0:128] * f[...]], axis=1)
        res[t * 128 : t * 128 + 128, :] = big_dot(turned)
        return unfold(t)

    def level_part(ph):
        with jax.named_scope("waitm%d" % ph):
            wait15(xm.at[ph], fmsem.at[ph])
        with jax.named_scope("main%d" % ph):
            store_spec(0, dft16([(get_main(ph, d, 0), get_main(ph, d, 1)) for d in range(16)]))
            spec = big_dot(lhs[0:128, :])
            own_spec = spec.reshape(16, 8, 256)
            fa = filtered(0, spec, fo)
            for d in range(16):
                for l in range(2):
                    x, nx, pv_ = fa[d][l], fa[(d + 1) % 16][l], fa[(d + 15) % 16][l]
                    r2 = pltpu.roll(jnp.where(lane < 2, nx, x), 126, 1)
                    l2 = pltpu.roll(jnp.where(lane >= 126, pv_, x), 2, 1)
                    dsend[ph, d, l] = -zc * zc * ((r2 - x) - (x - l2))
                    if ph == SUBSTEPS - 1:
                        r1 = pltpu.roll(jnp.where(lane < 1, nx, x), 127, 1)
                        l1 = pltpu.roll(jnp.where(lane >= 127, pv_, x), 1, 1)
                        du[d, l] = -zc * (r1 - l1)
            if ph == SUBSTEPS - 1:
                backward(du, ru, 12, bksem.at[2])
        with jax.named_scope("waite%d" % ph):
            wait_all(xe.at[ph, :, :, 0:2], fesem.at[ph, 0])
            wait_all(xe.at[ph, :, :, 0:2], fesem.at[ph, 1])
        with jax.named_scope("edge%d" % ph):
            store_spec(1, dft16([(get_edge(ph, d, 0), get_edge(ph, d, 1)) for d in range(16)]))
            edge_spec = big_dot(lhs[128:256, :]).reshape(16, 8, 256)
            wide = lax.broadcasted_iota(jnp.int32, (8, 256), 0)
            bt, ht = [], []
            for k1 in range(16):
                o, e = own_spec[k1], edge_spec[k1]
                ou, od = pltpu.roll(o, 7, 0), pltpu.roll(o, 1, 0)
                eu_, ed_ = pltpu.roll(e, 7, 0), pltpu.roll(e, 1, 0)
                bt.append(jnp.where(wide == 7, eu_, ou) - jnp.where(wide == 0, ed_, od))
                ht.append(jnp.where(wide == 0, eu_ - od, ou - ed_))
            hv = filtered(2, jnp.concatenate(ht, axis=0), fh)
            dy = filtered(1, jnp.concatenate(bt, axis=0), fb)
            for d in range(16):
                for l in range(2):
                    x, e = dy[d][l], hv[d][l]
                    north = pltpu.roll(jnp.where(sub == 0, e, x), 7, 0)
                    south = pltpu.roll(jnp.where(sub == 7, e, x), 1, 0)
                    dsend[ph, d, l] = dsend[ph, d, l] + mc * (north - south)
                    if ph == SUBSTEPS - 1:
                        dv[d, l] = x

    def column(ph, pin, win, pout, wout):
        ps = [pin[k] - sv[k] * (div0[k] + back[ph, k]) for k in range(NL)]
        vals = []
        pval = jnp.zeros((8, 128), F32)
        for k in range(NL):
            al = a_s[k]
            if k + 1 < NL:
                rhs = win[k] - al * (ps[k + 1] - ps[k])
            else:
                rhs = win[k] + al * ps[k]
            pval = rhs * inv[k] + qq[k] * pval
            vals.append(pval)
        wk = vals[-1]
        for k in range(NL - 1, -1, -1):
            wout[k] = wk
            if k:
                wlow = vals[k - 1] - rat[k - 1] * wk
                pout[k] = ps[k] - sv[k] * (wk - wlow)
                wk = wlow
            else:
                pout[k] = ps[k] - sv[k] * wk

    level_part(0)
    with jax.named_scope("bk0"):
        backward(dsend.at[0], back.at[0], 10, bksem.at[0])
    with jax.named_scope("waitb0"):
        wait30(back.at[0], bksem.at[0])
    with jax.named_scope("col0"):
        column(0, pv, wv, p1, w1)
    with jax.named_scope("fwd1"):
        forward(1, p1)
    level_part(1)
    with jax.named_scope("bk1"):
        backward(dsend.at[1], back.at[1], 11, bksem.at[1])
        backward(dv, rv, 13, bksem.at[3])
    with jax.named_scope("waitb1"):
        wait30(back.at[1], bksem.at[1])
    with jax.named_scope("col1"):
        column(1, p1, w1, p2, w2)
    with jax.named_scope("fin"):
        wait30(ru, bksem.at[2])
        for k in range(NL):
            uo[k] = ru[k] + uv[k]
        wait30(rv, bksem.at[3])
        for k in range(NL):
            vo[k] = rv[k] + vv[k]
    with jax.named_scope("sends"):
        for ph in range(SUBSTEPS):
            wait15(xm.at[ph], sendsem.at[3 * ph])
            wait_all(xe.at[ph, :, :, 0:2], sendsem.at[3 * ph + 1])
            wait_all(xe.at[ph, :, :, 0:2], sendsem.at[3 * ph + 2])
        wait_all(back.at[0, 0:2], sendsem.at[6])
        wait_all(back.at[0, 0:2], sendsem.at[7])
        wait_all(ev.at[:, 0:1], sendsem.at[8])
        wait_all(ev.at[:, 0:1], sendsem.at[9])
        for i in range(10, 14):
            wait30(ru, sendsem.at[i])

def store(u, v, w, p, uo, vo, wo, po, sem):
    copies = [pltpu.make_async_copy(a, b, sem.at[i]) for i, (a, b) in enumerate([(u, uo), (v, vo), (w, wo), (p, po)])]
    for c in copies:
        c.start()
    for c in copies:
        c.wait()


def solution(mesh):
    mat_np, tw_np = tables()
    field = jax.ShapeDtypeStruct((NL, 8, 128), F32)
    vmem = pl.BlockSpec(memory_space=pltpu.VMEM)
    hbm = pl.BlockSpec(memory_space=pltpu.HBM)
    blk = pltpu.VMEM((NL, 8, 128), F32)
    quad = pltpu.VMEM((2, 16, 2, 8, 128), F32)
    line = pltpu.VMEM((8, 128), F32)
    rows = pltpu.VMEM((384, 256), F32)
    dma = pltpu.SemaphoreType.DMA
    scratch = [
        blk, blk, blk, blk, blk, pltpu.VMEM((768, 256), jnp.bfloat16), pltpu.VMEM((2, 16, 128), F32),
        blk, blk, quad, quad, pltpu.VMEM((256, 256), F32), rows, quad, pltpu.VMEM((2, NL, 8, 128), F32),
        pltpu.VMEM((16, 2, 8, 128), F32), pltpu.VMEM((16, 2, 8, 128), F32), blk, blk,
        blk, blk, blk, blk, line, line, line, blk, line, line, line,
        pltpu.VMEM((128, 128), F32), pltpu.VMEM((128, 128), F32), pltpu.VMEM((128, 128), F32),
        pltpu.SMEM((8,), F32), pltpu.SMEM((8,), F32), pltpu.SMEM((NL,), F32), pltpu.SMEM((64,), jnp.int32), pltpu.SMEM((64,), jnp.int32),
        dma((7,)), dma((5,)), dma((14,)), dma((2,)), dma((2, 2)), dma((4,)), dma((6,)),
    ]
    call = pl.pallas_call(
        kernel,
        out_shape=(blk,) * 4,
        in_specs=[hbm] * 12,
        out_specs=(vmem,) * 4,
        scratch_shapes=scratch,
        compiler_params=pltpu.CompilerParams(collective_id=0, has_side_effects=True),
    )

    finish = pl.pallas_call(
        store, out_shape=(field,) * 4, in_specs=[vmem] * 4, out_specs=(hbm,) * 4, scratch_shapes=[dma((4,))]
    )

    def hold(*xs):
        return [pltpu.with_memory_space_constraint(o, pltpu.VMEM) for o in call(*xs)]

    def body(u, v, w, p, zc, mc, a, s, cutoff, mask):
        return finish(*hold(zc, mc, a, cutoff, mask, u, v, w, p, s, jnp.asarray(mat_np), jnp.asarray(tw_np)))

    f = P(None, "lat", "lon")
    return jax.shard_map(
        body,
        mesh=mesh,
        in_specs=(f, f, f, f, P("lat"), P("lat"), P(None), f, P(None), P(None)),
        out_specs=(f,) * 4,
        check_vma=False,
    )
```

```python
import math

import jax
import jax.numpy as jnp
import numpy as np
from jax import lax
from jax.experimental import pallas as pl
from jax.experimental.pallas import tpu as pltpu
from jax.sharding import PartitionSpec as P

SUBSTEPS = 2
F32 = jnp.float32
NG = 8
ND = 16
NL = 32
MESH = pl.DeviceIdType.MESH


def tables():
    lane = np.arange(128)
    ang = 2.0 * np.pi * ((lane[:, None] * lane[None, :]) % 128) / 128.0
    c, s = np.cos(ang), np.sin(ang)
    mat = np.block([[c, -s], [s, c]])
    high = mat.astype(np.float32).astype(jnp.bfloat16)
    low = (mat - high.astype(np.float64)).astype(np.float32).astype(jnp.bfloat16)
    mat = np.concatenate([high, high, low])
    tang = 2.0 * np.pi * (np.arange(16)[:, None] * lane[None, :]) / 2048.0
    tw = np.stack([np.cos(tang), -np.sin(tang)]).astype(np.float32)
    return mat, tw


def dft4(x):
    (ar, ai), (br, bi), (cr, ci), (dr, di) = x
    sr, si = ar + cr, ai + ci
    tr, ti = ar - cr, ai - ci
    ur, ui = br + dr, bi + di
    vr, vi = br - dr, bi - di
    return [(sr + ur, si + ui), (tr + vi, ti - vr), (sr - ur, si - ui), (tr - vi, ti + vr)]


def dft16(x):
    cols = []
    for n2 in range(4):
        y = dft4([x[4 * n1 + n2] for n1 in range(4)])
        out = []
        for k1 in range(4):
            e = (n2 * k1) % 16
            yr, yi = y[k1]
            if e == 0:
                out.append((yr, yi))
            elif e == 4:
                out.append((yi, -yr))
            else:
                c, s = math.cos(2 * math.pi * e / 16), math.sin(2 * math.pi * e / 16)
                out.append((yr * c + yi * s, yi * c - yr * s))
        cols.append(out)
    res = [None] * 16
    for k1 in range(4):
        z = dft4([cols[n2][k1] for n2 in range(4)])
        for k2 in range(4):
            res[k1 + 4 * k2] = z[k2]
    return res


def hops(off):
    return sum(min(o, 4 - o) for o in off)


OFFS = sorted([(a, b) for a in range(4) for b in range(4)], key=lambda o: -hops(o))


def kernel(
    zc_h, mc_h, a_h, cut_h, msk_h, u_h, v_h, w_h, p_h, s_h, mat_h, tw_h,
    uo, vo, w2, p2,
    uv, vv, wv, pv, sv, mat, tw, p1, w1, xm, xe, lhs, res, dsend, back,
    du, dv, ru, rv, rat, inv, qq, div0, eu, eul, eur, ev, mct, mcp, mcn, fo, fb, fh,
    zc_s, mc_s, a_s, cut_s, msk_s,
    ldsem, smsem, sendsem, fmsem, fesem, bksem, esem,
):
    me = lax.axis_index("lon")
    g = lax.axis_index("lat")
    par = g % 2
    up = (g + 1) % NG
    dn = (g + NG - 1) % NG
    my, mx = me // 4, me % 4
    east = (me + 1) % ND
    west = (me + ND - 1) % ND

    loads = [
        pltpu.make_async_copy(a, b, ldsem.at[i])
        for i, (a, b) in enumerate(
            [(p_h, pv), (u_h, uv), (v_h, vv), (s_h, sv), (w_h, wv), (tw_h, tw), (mat_h, mat)]
        )
    ]
    small = [
        pltpu.make_async_copy(a, b, smsem.at[i])
        for i, (a, b) in enumerate(
            [(zc_h, zc_s), (mc_h, mc_s), (a_h, a_s), (cut_h, cut_s), (msk_h, msk_s)]
        )
    ]
    bar = pltpu.get_barrier_semaphore()

    def target(off):
        return ((my + off[0]) % 4) * 4 + (mx + off[1]) % 4

    for off in OFFS:
        d = target(off)
        pl.semaphore_signal(bar, inc=1, device_id={"lat": up, "lon": d}, device_id_type=MESH)
        pl.semaphore_signal(bar, inc=1, device_id={"lat": dn, "lon": d}, device_id_type=MESH)
        if off != (0, 0):
            pl.semaphore_signal(bar, inc=1, device_id={"lat": g, "lon": d}, device_id_type=MESH)

    for c in loads[:1] + small + loads[1:]:
        c.start()

    def rcopy(src, dst, si, sem, gg, d):
        c = pltpu.make_async_remote_copy(
            src_ref=src, dst_ref=dst, send_sem=sendsem.at[si], recv_sem=sem,
            device_id={"lat": gg, "lon": d}, device_id_type=MESH,
        )
        c.start()

    def forward(ph, src):
        for off in OFFS:
            d = target(off)
            rcopy(src.at[pl.ds(2 * d, 2), 6:8], xe.at[ph, me, :, 6:8], 3 * ph + 1, fesem.at[ph, 0], up, d)
            rcopy(src.at[pl.ds(2 * d, 2), 0:2], xe.at[ph, me, :, 0:2], 3 * ph + 2, fesem.at[ph, 1], dn, d)
        for off in OFFS:
            d = target(off)
            if off != (0, 0):
                rcopy(src.at[pl.ds(2 * d, 2)], xm.at[ph, me], 3 * ph, fmsem.at[ph], g, d)
        xm[ph, pl.ds(me, 1)] = src[pl.ds(2 * me, 2)][None]

    def wait15(buf, sem):
        pltpu.make_async_copy(buf.at[pl.ds(0, 15)], buf.at[pl.ds(0, 15)], sem).wait()

    def wait_all(buf, sem):
        pltpu.make_async_copy(buf, buf, sem).wait()

    sub = lax.broadcasted_iota(jnp.int32, (8, 128), 0)
    lane = lax.broadcasted_iota(jnp.int32, (8, 128), 1)

    def tile(read):
        t = jnp.full((8, 128), read(0))
        for r in range(1, 8):
            t = jnp.where(sub == r, read(r), t)
        return t

    valid = jnp.logical_or(
        jnp.logical_and(sub >= 4, jnp.full((8, 128), g) > 0),
        jnp.logical_and(sub < 4, jnp.full((8, 128), g) < NG - 1),
    )

    with jax.named_scope("entry"):
        loads[0].wait()
        for c in small:
            c.wait()
        zc = tile(lambda r: zc_s[r])
        mc = tile(lambda r: mc_s[r])
        mct[...] = mc
        own = lambda ref: tile(lambda r: ref[8 * g + r])
        halo = lambda ref: jnp.where(sub == 0, ref[(8 * g + 8) % 64], ref[(8 * g + 63) % 64])
        pl.semaphore_wait(bar, 47)
    with jax.named_scope("fwd0"):
        rcopy(mct, mcp, 6, esem.at[0], up, me)
        rcopy(mct, mcn, 6, esem.at[1], dn, me)
        forward(0, pv)
    with jax.named_scope("home"):
        loads[1].wait()
        e = jnp.zeros((8, 128), F32)
        for k in range(NL):
            uk = uv[k]
            e = jnp.where(lane == k, pltpu.roll(uk, (k + 1) % 128, 1), e)
            e = jnp.where(lane == 32 + k, pltpu.roll(uk, 32 + k, 1), e)
        eu[...] = e
        rcopy(eu, eul, 7, esem.at[2], g, east)
        rcopy(eu, eur, 7, esem.at[3], g, west)
        loads[2].wait()
        rcopy(vv.at[:, 7:8], ev.at[:, 7:8], 8, esem.at[4], up, me)
        rcopy(vv.at[:, 0:1], ev.at[:, 0:1], 9, esem.at[5], dn, me)

        def factors(cut, mask):
            k1 = lax.broadcasted_iota(jnp.int32, (16, 8, 128), 0)
            k2 = lax.broadcasted_iota(jnp.int32, (16, 8, 128), 2)
            k = k1 + 16 * k2
            kk = jnp.minimum(k, 2048 - k).astype(F32)
            c = cut.astype(F32)[None]
            ratio = c / jnp.maximum(kk, 1.0)
            damped = jnp.logical_and(kk > c, mask[None] > 0)
            return jnp.where(damped, ratio * ratio, 1.0) * (1.0 / 2048.0)

        fo[...] = factors(own(cut_s), own(msk_s)).reshape(128, 128)
        fb[...] = (-mc[None] * factors(own(cut_s), own(msk_s))).reshape(128, 128)

        wait_all(mcp, esem.at[0])
        wait_all(mcn, esem.at[1])
        mch = jnp.where(sub >= 4, mcp[...], mcn[...])
        mch = jnp.where(valid, mch, 0.0)
        fh[...] = (-mch[None] * factors(halo(cut_s), halo(msk_s))).reshape(128, 128)
    loads[5].wait()
    loads[6].wait()

    def get_main(ph, d, l):
        x = xm[0, d, l]
        return x + xm[1, d, l] if ph else x

    def get_edge(ph, d, l):
        x = xe[0, d, l]
        x = x + xe[1, d, l] if ph else x
        return jnp.where(valid, x, 0.0)

    def store_spec(t, spec):
        for k1 in range(16):
            r, i = spec[k1]
            tr, ti = tw[0, k1 : k1 + 1, :], tw[1, k1 : k1 + 1, :]
            row = t * 128 + k1 * 8
            lhs[row : row + 8, 0:128] = r * tr - i * ti
            lhs[row : row + 8, 128:256] = r * ti + i * tr

    def big_dot(x):
        high = x.astype(jnp.bfloat16)
        low = (x - high.astype(F32)).astype(jnp.bfloat16)
        one = lambda a, b: jnp.dot(a, b, preferred_element_type=F32)
        return one(jnp.concatenate([high, low, high], axis=1), mat[...])

    def unfold(t):
        x = []
        for k1 in range(16):
            row = t * 128 + k1 * 8
            r, i = res[row : row + 8, 0:128], res[row : row + 8, 128:256]
            tr, ti = tw[0, k1 : k1 + 1, :], tw[1, k1 : k1 + 1, :]
            x.append((r * tr - i * ti, r * ti + i * tr))
        return [(b, a) for a, b in dft16(x)]

    def backward(src, dst, si, sem):
        for off in OFFS:
            d = target(off)
            if off != (0, 0):
                rcopy(src.at[d], dst.at[pl.ds(2 * me, 2)], si, sem, g, d)
        dst[pl.ds(2 * me, 2)] = src[pl.ds(me, 1)][0]

    def wait30(buf, sem):
        pltpu.make_async_copy(buf.at[pl.ds(0, 30)], buf.at[pl.ds(0, 30)], sem).wait()

    def filtered(t, spec, f):
        turned = jnp.concatenate([spec[:, 128:256] * f[...], spec[:, 0:128] * f[...]], axis=1)
        res[t * 128 : t * 128 + 128, :] = big_dot(turned)
        return unfold(t)

    def zonal_part(ph, fa):
        for d in range(16):
            for l in range(2):
                x, nx, pv_ = fa[d][l], fa[(d + 1) % 16][l], fa[(d + 15) % 16][l]
                r2 = pltpu.roll(jnp.where(lane < 2, nx, x), 126, 1)
                l2 = pltpu.roll(jnp.where(lane >= 126, pv_, x), 2, 1)
                dsend[ph, d, l] = -zc * zc * ((r2 - x) - (x - l2))
                if ph == SUBSTEPS - 1:
                    r1 = pltpu.roll(jnp.where(lane < 1, nx, x), 127, 1)
                    l1 = pltpu.roll(jnp.where(lane >= 127, pv_, x), 1, 1)
                    du[d, l] = -zc * (r1 - l1)

    def merid_spectra(own_spec, edge_spec):
        wide = lax.broadcasted_iota(jnp.int32, (8, 256), 0)
        bt, ht = [], []
        for k1 in range(16):
            o, e = own_spec[k1], edge_spec[k1]
            ou, od = pltpu.roll(o, 7, 0), pltpu.roll(o, 1, 0)
            eu_, ed_ = pltpu.roll(e, 7, 0), pltpu.roll(e, 1, 0)
            bt.append(jnp.where(wide == 7, eu_, ou) - jnp.where(wide == 0, ed_, od))
            ht.append(jnp.where(wide == 0, eu_ - od, ou - ed_))
        return jnp.concatenate(bt, axis=0), jnp.concatenate(ht, axis=0)

    def merid_part(ph, dy, hv):
        for d in range(16):
            for l in range(2):
                x, e = dy[d][l], hv[d][l]
                north = pltpu.roll(jnp.where(sub == 0, e, x), 7, 0)
                south = pltpu.roll(jnp.where(sub == 7, e, x), 1, 0)
                dsend[ph, d, l] = dsend[ph, d, l] + mc * (north - south)
                if ph == SUBSTEPS - 1:
                    dv[d, l] = x

    def wait_edges(ph):
        wait_all(xe.at[ph, :, :, 0:2], fesem.at[ph, 0])
        wait_all(xe.at[ph, :, :, 0:2], fesem.at[ph, 1])

    def fold_main(ph):
        store_spec(0, dft16([(get_main(ph, d, 0), get_main(ph, d, 1)) for d in range(16)]))

    def fold_edge(ph):
        store_spec(1, dft16([(get_edge(ph, d, 0), get_edge(ph, d, 1)) for d in range(16)]))

    def whole(ph):
        fold_main(ph)
        fold_edge(ph)
        spec = big_dot(lhs[...])
        bt, ht = merid_spectra(spec[0:128].reshape(16, 8, 256), spec[128:256].reshape(16, 8, 256))
        fa = filtered(0, spec[0:128], fo)
        hv = filtered(2, ht, fh)
        dy = filtered(1, bt, fb)
        zonal_part(ph, fa)
        merid_part(ph, dy, hv)

    def parted(ph):
        fold_main(ph)
        spec = big_dot(lhs[0:128, :])
        zonal_part(ph, filtered(0, spec, fo))
        if ph == SUBSTEPS - 1:
            backward(du, ru, 12, bksem.at[2])
        with jax.named_scope("waite%d" % ph):
            wait_edges(ph)
        with jax.named_scope("edge%d" % ph):
            fold_edge(ph)
            bt, ht = merid_spectra(spec.reshape(16, 8, 256), big_dot(lhs[128:256, :]).reshape(16, 8, 256))
            hv = filtered(2, ht, fh)
            dy = filtered(1, bt, fb)
            merid_part(ph, dy, hv)

    def level_part(ph):
        with jax.named_scope("waitm%d" % ph):
            wait15(xm.at[ph], fmsem.at[ph])

        @pl.when(par == 0)
        def _():
            wait_edges(ph)
            with jax.named_scope("whole%d" % ph):
                whole(ph)
            if ph == SUBSTEPS - 1:
                backward(du, ru, 12, bksem.at[2])

        @pl.when(par == 1)
        def _():
            parted(ph)

    def column(ph, pin, win, pout, wout):
        ps = [pin[k] - sv[k] * (div0[k] + back[ph, k]) for k in range(NL)]
        vals = []
        pval = jnp.zeros((8, 128), F32)
        for k in range(NL):
            al = a_s[k]
            if k + 1 < NL:
                rhs = win[k] - al * (ps[k + 1] - ps[k])
            else:
                rhs = win[k] + al * ps[k]
            pval = rhs * inv[k] + qq[k] * pval
            vals.append(pval)
        wk = vals[-1]
        for k in range(NL - 1, -1, -1):
            wout[k] = wk
            if k:
                wlow = vals[k - 1] - rat[k - 1] * wk
                pout[k] = ps[k] - sv[k] * (wk - wlow)
                wk = wlow
            else:
                pout[k] = ps[k] - sv[k] * wk

    level_part(0)
    with jax.named_scope("bk0"):
        backward(dsend.at[0], back.at[0], 10, bksem.at[0])
    with jax.named_scope("home2"):
        loads[3].wait()
        prev = jnp.zeros((8, 128), F32)
        for k in range(NL):
            al = a_s[k]
            below = al * sv[k]
            above = al * sv[k + 1] if k + 1 < NL else jnp.zeros((8, 128), F32)
            ip = 1.0 / (1.0 + below + above + below * prev)
            prev = -above * ip
            rat[k] = prev
            inv[k] = ip
            qq[k] = below * ip

        wait_all(eul, esem.at[2])
        wait_all(eur, esem.at[3])
        wait_all(ev.at[:, 7:8], esem.at[4])
        wait_all(ev.at[:, 0:1], esem.at[5])
        el, er = eul[...], eur[...]
        for k in range(NL):
            uk, vk = uv[k], vv[k]
            evk = jnp.where(valid, ev[k], 0.0)
            right = jnp.where(lane == 127, pltpu.roll(er, (95 - k) % 128, 1), pltpu.roll(uk, 127, 1))
            left = jnp.where(lane == 0, pltpu.roll(el, (128 - k) % 128, 1), pltpu.roll(uk, 1, 1))
            north = pltpu.roll(jnp.where(sub == 0, evk, vk), 7, 0)
            south = pltpu.roll(jnp.where(sub == 7, evk, vk), 1, 0)
            div0[k] = zc * (right - left) + mc * (north - south)
        loads[4].wait()
    with jax.named_scope("waitb0"):
        wait30(back.at[0], bksem.at[0])
    with jax.named_scope("col0"):
        column(0, pv, wv, p1, w1)
    with jax.named_scope("fwd1"):
        forward(1, p1)
    level_part(1)
    with jax.named_scope("bk1"):
        backward(dsend.at[1], back.at[1], 11, bksem.at[1])
        backward(dv, rv, 13, bksem.at[3])
    with jax.named_scope("waitb1"):
        wait30(back.at[1], bksem.at[1])
    with jax.named_scope("col1"):
        column(1, p1, w1, p2, w2)
    with jax.named_scope("fin"):
        wait30(ru, bksem.at[2])
        for k in range(NL):
            uo[k] = ru[k] + uv[k]
        wait30(rv, bksem.at[3])
        for k in range(NL):
            vo[k] = rv[k] + vv[k]
    with jax.named_scope("sends"):
        for ph in range(SUBSTEPS):
            wait15(xm.at[ph], sendsem.at[3 * ph])
            wait_all(xe.at[ph, :, :, 0:2], sendsem.at[3 * ph + 1])
            wait_all(xe.at[ph, :, :, 0:2], sendsem.at[3 * ph + 2])
        wait_all(back.at[0, 0:2], sendsem.at[6])
        wait_all(back.at[0, 0:2], sendsem.at[7])
        wait_all(ev.at[:, 0:1], sendsem.at[8])
        wait_all(ev.at[:, 0:1], sendsem.at[9])
        for i in range(10, 14):
            wait30(ru, sendsem.at[i])

def store(u, v, w, p, uo, vo, wo, po, sem):
    copies = [pltpu.make_async_copy(a, b, sem.at[i]) for i, (a, b) in enumerate([(u, uo), (v, vo), (w, wo), (p, po)])]
    for c in copies:
        c.start()
    for c in copies:
        c.wait()


def solution(mesh):
    mat_np, tw_np = tables()
    field = jax.ShapeDtypeStruct((NL, 8, 128), F32)
    vmem = pl.BlockSpec(memory_space=pltpu.VMEM)
    hbm = pl.BlockSpec(memory_space=pltpu.HBM)
    blk = pltpu.VMEM((NL, 8, 128), F32)
    quad = pltpu.VMEM((2, 16, 2, 8, 128), F32)
    line = pltpu.VMEM((8, 128), F32)
    rows = pltpu.VMEM((384, 256), F32)
    dma = pltpu.SemaphoreType.DMA
    scratch = [
        blk, blk, blk, blk, blk, pltpu.VMEM((768, 256), jnp.bfloat16), pltpu.VMEM((2, 16, 128), F32),
        blk, blk, quad, quad, pltpu.VMEM((256, 256), F32), rows, quad, pltpu.VMEM((2, NL, 8, 128), F32),
        pltpu.VMEM((16, 2, 8, 128), F32), pltpu.VMEM((16, 2, 8, 128), F32), blk, blk,
        blk, blk, blk, blk, line, line, line, blk, line, line, line,
        pltpu.VMEM((128, 128), F32), pltpu.VMEM((128, 128), F32), pltpu.VMEM((128, 128), F32),
        pltpu.SMEM((8,), F32), pltpu.SMEM((8,), F32), pltpu.SMEM((NL,), F32), pltpu.SMEM((64,), jnp.int32), pltpu.SMEM((64,), jnp.int32),
        dma((7,)), dma((5,)), dma((14,)), dma((2,)), dma((2, 2)), dma((4,)), dma((6,)),
    ]
    call = pl.pallas_call(
        kernel,
        out_shape=(blk,) * 4,
        in_specs=[hbm] * 12,
        out_specs=(vmem,) * 4,
        scratch_shapes=scratch,
        compiler_params=pltpu.CompilerParams(collective_id=0, has_side_effects=True),
    )

    finish = pl.pallas_call(
        store, out_shape=(field,) * 4, in_specs=[vmem] * 4, out_specs=(hbm,) * 4, scratch_shapes=[dma((4,))]
    )

    def hold(*xs):
        return [pltpu.with_memory_space_constraint(o, pltpu.VMEM) for o in call(*xs)]

    def body(u, v, w, p, zc, mc, a, s, cutoff, mask):
        return finish(*hold(zc, mc, a, cutoff, mask, u, v, w, p, s, jnp.asarray(mat_np), jnp.asarray(tw_np)))

    f = P(None, "lat", "lon")
    return jax.shard_map(
        body,
        mesh=mesh,
        in_specs=(f, f, f, f, P("lat"), P("lat"), P(None), f, P(None), P(None)),
        out_specs=(f,) * 4,
        check_vma=False,
    )
```

```python
import math

import jax
import jax.numpy as jnp
import numpy as np
from jax import lax
from jax.experimental import pallas as pl
from jax.experimental.pallas import tpu as pltpu
from jax.sharding import PartitionSpec as P

SUBSTEPS = 2
F32 = jnp.float32
NG = 8
ND = 16
NL = 32
MESH = pl.DeviceIdType.MESH


def tables():
    lane = np.arange(128)
    ang = 2.0 * np.pi * ((lane[:, None] * lane[None, :]) % 128) / 128.0
    c, s = np.cos(ang), np.sin(ang)
    mat = np.block([[c, -s], [s, c]])
    high = mat.astype(np.float32).astype(jnp.bfloat16)
    low = (mat - high.astype(np.float64)).astype(np.float32).astype(jnp.bfloat16)
    mat = np.concatenate([high, high, low])
    tang = 2.0 * np.pi * (np.arange(16)[:, None] * lane[None, :]) / 2048.0
    theta = 2.0 * np.pi * (np.arange(16)[:, None] + 16 * lane[None, :]) / 2048.0
    tw = np.stack([np.cos(tang), -np.sin(tang), 2.0 * np.sin(theta)]).astype(np.float32)
    return mat, tw


def dft4(x):
    (ar, ai), (br, bi), (cr, ci), (dr, di) = x
    sr, si = ar + cr, ai + ci
    tr, ti = ar - cr, ai - ci
    ur, ui = br + dr, bi + di
    vr, vi = br - dr, bi - di
    return [(sr + ur, si + ui), (tr + vi, ti - vr), (sr - ur, si - ui), (tr - vi, ti + vr)]


def dft16(x):
    cols = []
    for n2 in range(4):
        y = dft4([x[4 * n1 + n2] for n1 in range(4)])
        out = []
        for k1 in range(4):
            e = (n2 * k1) % 16
            yr, yi = y[k1]
            if e == 0:
                out.append((yr, yi))
            elif e == 4:
                out.append((yi, -yr))
            else:
                c, s = math.cos(2 * math.pi * e / 16), math.sin(2 * math.pi * e / 16)
                out.append((yr * c + yi * s, yi * c - yr * s))
        cols.append(out)
    res = [None] * 16
    for k1 in range(4):
        z = dft4([cols[n2][k1] for n2 in range(4)])
        for k2 in range(4):
            res[k1 + 4 * k2] = z[k2]
    return res


def hops(off):
    return sum(min(o, 4 - o) for o in off)


OFFS = sorted([(a, b) for a in range(4) for b in range(4)], key=lambda o: -hops(o))


def kernel(
    zc_h, mc_h, a_h, cut_h, msk_h, u_h, v_h, w_h, p_h, s_h, mat_h, tw_h,
    uo, vo, w2, p2,
    uv, vv, wv, pv, sv, mat, tw, p1, w1, xm, xe, lhs, res, dsend, back,
    du, dv, ru, rv, rat, inv, qq, div0, eu, eul, eur, ev, mct, mcp, mcn, fo, fb, fd, fn, fs,
    zc_s, mc_s, a_s, cut_s, msk_s,
    ldsem, smsem, sendsem, fmsem, fesem, bksem, esem,
):
    me = lax.axis_index("lon")
    g = lax.axis_index("lat")
    par = g % 2
    up = (g + 1) % NG
    dn = (g + NG - 1) % NG
    my, mx = me // 4, me % 4
    east = (me + 1) % ND
    west = (me + ND - 1) % ND

    loads = [
        pltpu.make_async_copy(a, b, ldsem.at[i])
        for i, (a, b) in enumerate(
            [(p_h, pv), (u_h, uv), (v_h, vv), (s_h, sv), (w_h, wv), (tw_h, tw), (mat_h, mat)]
        )
    ]
    small = [
        pltpu.make_async_copy(a, b, smsem.at[i])
        for i, (a, b) in enumerate(
            [(zc_h, zc_s), (mc_h, mc_s), (a_h, a_s), (cut_h, cut_s), (msk_h, msk_s)]
        )
    ]
    bar = pltpu.get_barrier_semaphore()

    def target(off):
        return ((my + off[0]) % 4) * 4 + (mx + off[1]) % 4

    for off in OFFS:
        d = target(off)
        pl.semaphore_signal(bar, inc=1, device_id={"lat": up, "lon": d}, device_id_type=MESH)
        pl.semaphore_signal(bar, inc=1, device_id={"lat": dn, "lon": d}, device_id_type=MESH)
        if off != (0, 0):
            pl.semaphore_signal(bar, inc=1, device_id={"lat": g, "lon": d}, device_id_type=MESH)

    for c in loads[:1] + small + loads[1:]:
        c.start()

    def rcopy(src, dst, si, sem, gg, d):
        c = pltpu.make_async_remote_copy(
            src_ref=src, dst_ref=dst, send_sem=sendsem.at[si], recv_sem=sem,
            device_id={"lat": gg, "lon": d}, device_id_type=MESH,
        )
        c.start()

    def forward(ph, src):
        for off in OFFS:
            d = target(off)
            rcopy(src.at[pl.ds(2 * d, 2), 6:8], xe.at[ph, me, :, 6:8], 3 * ph + 1, fesem.at[ph, 0], up, d)
            rcopy(src.at[pl.ds(2 * d, 2), 0:2], xe.at[ph, me, :, 0:2], 3 * ph + 2, fesem.at[ph, 1], dn, d)
        for off in OFFS:
            d = target(off)
            if off != (0, 0):
                rcopy(src.at[pl.ds(2 * d, 2)], xm.at[ph, me], 3 * ph, fmsem.at[ph], g, d)
        xm[ph, pl.ds(me, 1)] = src[pl.ds(2 * me, 2)][None]

    def wait15(buf, sem):
        pltpu.make_async_copy(buf.at[pl.ds(0, 15)], buf.at[pl.ds(0, 15)], sem).wait()

    def wait_all(buf, sem):
        pltpu.make_async_copy(buf, buf, sem).wait()

    sub = lax.broadcasted_iota(jnp.int32, (8, 128), 0)
    lane = lax.broadcasted_iota(jnp.int32, (8, 128), 1)

    def tile(read):
        t = jnp.full((8, 128), read(0))
        for r in range(1, 8):
            t = jnp.where(sub == r, read(r), t)
        return t

    valid = jnp.logical_or(
        jnp.logical_and(sub >= 4, jnp.full((8, 128), g) > 0),
        jnp.logical_and(sub < 4, jnp.full((8, 128), g) < NG - 1),
    )

    with jax.named_scope("entry"):
        loads[0].wait()
        for c in small:
            c.wait()
        zc = tile(lambda r: zc_s[r])
        mc = tile(lambda r: mc_s[r])
        mct[...] = mc
        own = lambda ref: tile(lambda r: ref[8 * g + r])
        halo = lambda ref: jnp.where(sub == 0, ref[(8 * g + 8) % 64], ref[(8 * g + 63) % 64])
        pl.semaphore_wait(bar, 47)
    with jax.named_scope("fwd0"):
        rcopy(mct, mcp, 6, esem.at[0], up, me)
        rcopy(mct, mcn, 6, esem.at[1], dn, me)
        forward(0, pv)
    with jax.named_scope("home"):
        loads[1].wait()
        e = jnp.zeros((8, 128), F32)
        for k in range(NL):
            uk = uv[k]
            e = jnp.where(lane == k, pltpu.roll(uk, (k + 1) % 128, 1), e)
            e = jnp.where(lane == 32 + k, pltpu.roll(uk, 32 + k, 1), e)
        eu[...] = e
        rcopy(eu, eul, 7, esem.at[2], g, east)
        rcopy(eu, eur, 7, esem.at[3], g, west)
        loads[2].wait()
        rcopy(vv.at[:, 7:8], ev.at[:, 7:8], 8, esem.at[4], up, me)
        rcopy(vv.at[:, 0:1], ev.at[:, 0:1], 9, esem.at[5], dn, me)

        def factors(cut, mask):
            k1 = lax.broadcasted_iota(jnp.int32, (16, 8, 128), 0)
            k2 = lax.broadcasted_iota(jnp.int32, (16, 8, 128), 2)
            k = k1 + 16 * k2
            kk = jnp.minimum(k, 2048 - k).astype(F32)
            c = cut.astype(F32)[None]
            ratio = c / jnp.maximum(kk, 1.0)
            damped = jnp.logical_and(kk > c, mask[None] > 0)
            return jnp.where(damped, ratio * ratio, 1.0) * (1.0 / 2048.0)

        loads[5].wait()
        loads[6].wait()
        plain = factors(own(cut_s), own(msk_s))
        fb[...] = (-mc[None] * plain).reshape(128, 128)
        for k1 in range(16):
            wave = zc * tw[2, k1 : k1 + 1, :]
            fo[k1 * 8 : k1 * 8 + 8, :] = -wave * plain[k1]
            fd[k1 * 8 : k1 * 8 + 8, :] = wave * wave * plain[k1]

        wait_all(mcp, esem.at[0])
        wait_all(mcn, esem.at[1])
        mch = jnp.where(sub >= 4, mcp[...], mcn[...])
        mch = jnp.where(valid, mch, 0.0)
        rim = -mch[None] * factors(halo(cut_s), halo(msk_s))
        for k1 in range(16):
            row = slice(k1 * 8, k1 * 8 + 8)
            b = fb[row, :]
            above = mc * pltpu.roll(jnp.where(sub == 0, rim[k1], b), 7, 0)
            below = mc * pltpu.roll(jnp.where(sub == 7, rim[k1], b), 1, 0)
            fn[row, :] = above
            fs[row, :] = below
            fd[row, :] = fd[row, :] - (above + below)
    def get_main(ph, d, l):
        x = xm[0, d, l]
        return x + xm[1, d, l] if ph else x

    def get_edge(ph, d, l):
        x = xe[0, d, l]
        x = x + xe[1, d, l] if ph else x
        return x

    def store_spec(t, spec):
        for k1 in range(16):
            r, i = spec[k1]
            tr, ti = tw[0, k1 : k1 + 1, :], tw[1, k1 : k1 + 1, :]
            row = t * 128 + k1 * 8
            lhs[row : row + 8, 0:128] = r * tr - i * ti
            lhs[row : row + 8, 128:256] = r * ti + i * tr

    def big_dot(x):
        high = x.astype(jnp.bfloat16)
        low = (x - high.astype(F32)).astype(jnp.bfloat16)
        one = lambda a, b: jnp.dot(a, b, preferred_element_type=F32)
        return one(jnp.concatenate([high, low, high], axis=1), mat[...])

    def unfold(t):
        x = []
        for k1 in range(16):
            row = t * 128 + k1 * 8
            r, i = res[row : row + 8, 0:128], res[row : row + 8, 128:256]
            tr, ti = tw[0, k1 : k1 + 1, :], tw[1, k1 : k1 + 1, :]
            x.append((r * tr - i * ti, r * ti + i * tr))
        return [(b, a) for a, b in dft16(x)]

    def backward(src, dst, si, sem):
        for off in OFFS:
            d = target(off)
            if off != (0, 0):
                rcopy(src.at[d], dst.at[pl.ds(2 * me, 2)], si, sem, g, d)
        dst[pl.ds(2 * me, 2)] = src[pl.ds(me, 1)][0]

    def wait30(buf, sem):
        pltpu.make_async_copy(buf.at[pl.ds(0, 30)], buf.at[pl.ds(0, 30)], sem).wait()

    def inverse(t, real, imag):
        res[t * 128 : t * 128 + 128, :] = big_dot(jnp.concatenate([imag, real], axis=1))
        return unfold(t)

    def zonal(spec):
        y = inverse(0, -(spec[:, 128:256] * fo[...]), spec[:, 0:128] * fo[...])
        for d in range(16):
            for l in range(2):
                du[d, l] = y[d][l]

    def merid(real, imag):
        y = inverse(1, real, imag)
        for d in range(16):
            for l in range(2):
                dv[d, l] = y[d][l]

    def diverge(ph, real, imag):
        y = inverse(2, real, imag)
        for d in range(16):
            for l in range(2):
                dsend[ph, d, l] = y[d][l]

    def div_spectra(own_spec, edge_spec):
        parts = []
        for half in (0, 128):
            out = []
            for k1 in range(16):
                row = slice(k1 * 8, k1 * 8 + 8)
                o, e = own_spec[row, half : half + 128], edge_spec[row, half : half + 128]
                e = jnp.where(valid, e, 0.0)
                north = pltpu.roll(jnp.where(sub < 2, e, o), 6, 0)
                south = pltpu.roll(jnp.where(sub >= 6, e, o), 2, 0)
                out.append(fd[row, :] * o + fn[row, :] * north + fs[row, :] * south)
            parts.append(jnp.concatenate(out, axis=0))
        return parts

    def dv_spectra(own_spec, edge_spec):
        parts = []
        for half in (0, 128):
            out = []
            for k1 in range(16):
                row = slice(k1 * 8, k1 * 8 + 8)
                o, e = own_spec[row, half : half + 128], edge_spec[row, half : half + 128]
                e = jnp.where(valid, e, 0.0)
                north = pltpu.roll(jnp.where(sub == 0, e, o), 7, 0)
                south = pltpu.roll(jnp.where(sub == 7, e, o), 1, 0)
                out.append(fb[row, :] * (north - south))
            parts.append(jnp.concatenate(out, axis=0))
        return parts

    def wait_edges(ph):
        wait_all(xe.at[ph, :, :, 0:2], fesem.at[ph, 0])
        wait_all(xe.at[ph, :, :, 0:2], fesem.at[ph, 1])

    def fold_main(ph):
        store_spec(0, dft16([(get_main(ph, d, 0), get_main(ph, d, 1)) for d in range(16)]))

    def fold_edge(ph):
        store_spec(1, dft16([(get_edge(ph, d, 0), get_edge(ph, d, 1)) for d in range(16)]))

    def send_du():
        backward(du, ru, 12, bksem.at[2])

    def send_dv():
        backward(dv, rv, 13, bksem.at[3])

    def send_div(ph):
        backward(dsend.at[ph], back.at[ph], 10 + ph, bksem.at[ph])

    def whole(ph):
        fold_main(ph)
        fold_edge(ph)
        spec = big_dot(lhs[...])
        diverge(ph, *div_spectra(spec[0:128], spec[128:256]))
        send_div(ph)
        if ph == SUBSTEPS - 1:
            zonal(spec[0:128])
            send_du()
            merid(*dv_spectra(spec[0:128], spec[128:256]))
            send_dv()

    def parted(ph):
        fold_main(ph)
        spec = big_dot(lhs[0:128, :])
        if ph == SUBSTEPS - 1:
            zonal(spec)
            send_du()
        with jax.named_scope("waite%d" % ph):
            wait_edges(ph)
        with jax.named_scope("edge%d" % ph):
            fold_edge(ph)
            edge_spec = big_dot(lhs[128:256, :])
            diverge(ph, *div_spectra(spec, edge_spec))
            send_div(ph)
            if ph == SUBSTEPS - 1:
                merid(*dv_spectra(spec, edge_spec))
                send_dv()

    def level_part(ph):
        with jax.named_scope("waitm%d" % ph):
            wait15(xm.at[ph], fmsem.at[ph])

        @pl.when(par == 0)
        def _():
            wait_edges(ph)
            with jax.named_scope("whole%d" % ph):
                whole(ph)

        @pl.when(par == 1)
        def _():
            parted(ph)

    def column(ph, pin, win, pout, wout):
        ps = [pin[k] - sv[k] * (div0[k] + back[ph, k]) for k in range(NL)]
        vals = []
        pval = jnp.zeros((8, 128), F32)
        for k in range(NL):
            al = a_s[k]
            if k + 1 < NL:
                rhs = win[k] - al * (ps[k + 1] - ps[k])
            else:
                rhs = win[k] + al * ps[k]
            pval = rhs * inv[k] + qq[k] * pval
            vals.append(pval)
        wk = vals[-1]
        for k in range(NL - 1, -1, -1):
            wout[k] = wk
            if k:
                wlow = vals[k - 1] - rat[k - 1] * wk
                pout[k] = ps[k] - sv[k] * (wk - wlow)
                wk = wlow
            else:
                pout[k] = ps[k] - sv[k] * wk

    level_part(0)
    with jax.named_scope("home2"):
        loads[3].wait()
        prev = jnp.zeros((8, 128), F32)
        for k in range(NL):
            al = a_s[k]
            below = al * sv[k]
            above = al * sv[k + 1] if k + 1 < NL else jnp.zeros((8, 128), F32)
            ip = 1.0 / (1.0 + below + above + below * prev)
            prev = -above * ip
            rat[k] = prev
            inv[k] = ip
            qq[k] = below * ip

        wait_all(eul, esem.at[2])
        wait_all(eur, esem.at[3])
        wait_all(ev.at[:, 7:8], esem.at[4])
        wait_all(ev.at[:, 0:1], esem.at[5])
        el, er = eul[...], eur[...]
        for k in range(NL):
            uk, vk = uv[k], vv[k]
            evk = jnp.where(valid, ev[k], 0.0)
            right = jnp.where(lane == 127, pltpu.roll(er, (95 - k) % 128, 1), pltpu.roll(uk, 127, 1))
            left = jnp.where(lane == 0, pltpu.roll(el, (128 - k) % 128, 1), pltpu.roll(uk, 1, 1))
            north = pltpu.roll(jnp.where(sub == 0, evk, vk), 7, 0)
            south = pltpu.roll(jnp.where(sub == 7, evk, vk), 1, 0)
            div0[k] = zc * (right - left) + mc * (north - south)
        loads[4].wait()
    with jax.named_scope("waitb0"):
        wait30(back.at[0], bksem.at[0])
    with jax.named_scope("col0"):
        column(0, pv, wv, p1, w1)
    with jax.named_scope("fwd1"):
        forward(1, p1)
    level_part(1)
    with jax.named_scope("waitb1"):
        wait30(back.at[1], bksem.at[1])
    with jax.named_scope("col1"):
        column(1, p1, w1, p2, w2)
    with jax.named_scope("fin"):
        wait30(ru, bksem.at[2])
        for k in range(NL):
            uo[k] = ru[k] + uv[k]
        wait30(rv, bksem.at[3])
        for k in range(NL):
            vo[k] = rv[k] + vv[k]
    with jax.named_scope("sends"):
        for ph in range(SUBSTEPS):
            wait15(xm.at[ph], sendsem.at[3 * ph])
            wait_all(xe.at[ph, :, :, 0:2], sendsem.at[3 * ph + 1])
            wait_all(xe.at[ph, :, :, 0:2], sendsem.at[3 * ph + 2])
        wait_all(back.at[0, 0:2], sendsem.at[6])
        wait_all(back.at[0, 0:2], sendsem.at[7])
        wait_all(ev.at[:, 0:1], sendsem.at[8])
        wait_all(ev.at[:, 0:1], sendsem.at[9])
        for i in range(10, 14):
            wait30(ru, sendsem.at[i])

def store(u, v, w, p, uo, vo, wo, po, sem):
    copies = [pltpu.make_async_copy(a, b, sem.at[i]) for i, (a, b) in enumerate([(u, uo), (v, vo), (w, wo), (p, po)])]
    for c in copies:
        c.start()
    for c in copies:
        c.wait()


def solution(mesh):
    mat_np, tw_np = tables()
    field = jax.ShapeDtypeStruct((NL, 8, 128), F32)
    vmem = pl.BlockSpec(memory_space=pltpu.VMEM)
    hbm = pl.BlockSpec(memory_space=pltpu.HBM)
    blk = pltpu.VMEM((NL, 8, 128), F32)
    quad = pltpu.VMEM((2, 16, 2, 8, 128), F32)
    line = pltpu.VMEM((8, 128), F32)
    rows = pltpu.VMEM((384, 256), F32)
    dma = pltpu.SemaphoreType.DMA
    scratch = [
        blk, blk, blk, blk, blk, pltpu.VMEM((768, 256), jnp.bfloat16), pltpu.VMEM((3, 16, 128), F32),
        blk, blk, quad, quad, pltpu.VMEM((256, 256), F32), rows, quad, pltpu.VMEM((2, NL, 8, 128), F32),
        pltpu.VMEM((16, 2, 8, 128), F32), pltpu.VMEM((16, 2, 8, 128), F32), blk, blk,
        blk, blk, blk, blk, line, line, line, blk, line, line, line,
        pltpu.VMEM((128, 128), F32), pltpu.VMEM((128, 128), F32), pltpu.VMEM((128, 128), F32), pltpu.VMEM((128, 128), F32), pltpu.VMEM((128, 128), F32),
        pltpu.SMEM((8,), F32), pltpu.SMEM((8,), F32), pltpu.SMEM((NL,), F32), pltpu.SMEM((64,), jnp.int32), pltpu.SMEM((64,), jnp.int32),
        dma((7,)), dma((5,)), dma((14,)), dma((2,)), dma((2, 2)), dma((4,)), dma((6,)),
    ]
    call = pl.pallas_call(
        kernel,
        out_shape=(blk,) * 4,
        in_specs=[hbm] * 12,
        out_specs=(vmem,) * 4,
        scratch_shapes=scratch,
        compiler_params=pltpu.CompilerParams(collective_id=0, has_side_effects=True),
    )

    finish = pl.pallas_call(
        store, out_shape=(field,) * 4, in_specs=[vmem] * 4, out_specs=(hbm,) * 4, scratch_shapes=[dma((4,))]
    )

    def hold(*xs):
        return [pltpu.with_memory_space_constraint(o, pltpu.VMEM) for o in call(*xs)]

    def body(u, v, w, p, zc, mc, a, s, cutoff, mask):
        return finish(*hold(zc, mc, a, cutoff, mask, u, v, w, p, s, jnp.asarray(mat_np), jnp.asarray(tw_np)))

    f = P(None, "lat", "lon")
    return jax.shard_map(
        body,
        mesh=mesh,
        in_specs=(f, f, f, f, P("lat"), P("lat"), P(None), f, P(None), P(None)),
        out_specs=(f,) * 4,
        check_vma=False,
    )
```

```python
import math

import jax
import jax.numpy as jnp
import numpy as np
from jax import lax
from jax.experimental import pallas as pl
from jax.experimental.pallas import tpu as pltpu
from jax.sharding import PartitionSpec as P

SUBSTEPS = 2
F32 = jnp.float32
NG = 8
ND = 16
NL = 32
MESH = pl.DeviceIdType.MESH


def tables():
    lane = np.arange(128)
    ang = 2.0 * np.pi * ((lane[:, None] * lane[None, :]) % 128) / 128.0
    c, s = np.cos(ang), np.sin(ang)
    mat = np.block([[c, -s], [s, c]])
    high = mat.astype(np.float32).astype(jnp.bfloat16)
    low = (mat - high.astype(np.float64)).astype(np.float32).astype(jnp.bfloat16)
    mat = np.concatenate([high, high, low])
    tang = 2.0 * np.pi * (np.arange(16)[:, None] * lane[None, :]) / 2048.0
    theta = 2.0 * np.pi * (np.arange(16)[:, None] + 16 * lane[None, :]) / 2048.0
    tw = np.stack([np.cos(tang), -np.sin(tang), 2.0 * np.sin(theta)]).astype(np.float32)
    return mat, tw


def dft4(x):
    (ar, ai), (br, bi), (cr, ci), (dr, di) = x
    sr, si = ar + cr, ai + ci
    tr, ti = ar - cr, ai - ci
    ur, ui = br + dr, bi + di
    vr, vi = br - dr, bi - di
    return [(sr + ur, si + ui), (tr + vi, ti - vr), (sr - ur, si - ui), (tr - vi, ti + vr)]


def dft16(x):
    cols = []
    for n2 in range(4):
        y = dft4([x[4 * n1 + n2] for n1 in range(4)])
        out = []
        for k1 in range(4):
            e = (n2 * k1) % 16
            yr, yi = y[k1]
            if e == 0:
                out.append((yr, yi))
            elif e == 4:
                out.append((yi, -yr))
            else:
                c, s = math.cos(2 * math.pi * e / 16), math.sin(2 * math.pi * e / 16)
                out.append((yr * c + yi * s, yi * c - yr * s))
        cols.append(out)
    res = [None] * 16
    for k1 in range(4):
        z = dft4([cols[n2][k1] for n2 in range(4)])
        for k2 in range(4):
            res[k1 + 4 * k2] = z[k2]
    return res


def hops(off):
    return sum(min(o, 4 - o) for o in off)


OFFS = sorted([(a, b) for a in range(4) for b in range(4)], key=lambda o: -hops(o))


def kernel(
    zc_h, mc_h, a_h, cut_h, msk_h, u_h, v_h, w_h, p_h, s_h, mat_h, tw_h,
    uo, vo, w2, p2,
    uv, vv, wv, pv, sv, mat, tw, p1, w1, xm, xe, lhs, res, dsend, back,
    du, dv, ru, rv, rat, inv, qq, div0, eu, eul, eur, ev, mct, mcp, mcn, fo, fb, fd, fn, fs,
    zc_s, mc_s, a_s, cut_s, msk_s,
    ldsem, smsem, sendsem, fmsem, fesem, bksem, esem, ready,
):
    me = lax.axis_index("lon")
    g = lax.axis_index("lat")
    par = g % 2
    up = (g + 1) % NG
    dn = (g + NG - 1) % NG
    my, mx = me // 4, me % 4
    east = (me + 1) % ND
    west = (me + ND - 1) % ND

    loads = [
        pltpu.make_async_copy(a, b, ldsem.at[i])
        for i, (a, b) in enumerate(
            [(p_h, pv), (u_h, uv), (v_h, vv), (s_h, sv), (w_h, wv), (tw_h, tw), (mat_h, mat)]
        )
    ]
    small = [
        pltpu.make_async_copy(a, b, smsem.at[i])
        for i, (a, b) in enumerate(
            [(zc_h, zc_s), (mc_h, mc_s), (a_h, a_s), (cut_h, cut_s), (msk_h, msk_s)]
        )
    ]
    bar = pltpu.get_barrier_semaphore()

    def target(off):
        return ((my + off[0]) % 4) * 4 + (mx + off[1]) % 4

    def tell(sem, gg, d):
        pl.semaphore_signal(sem, inc=1, device_id={"lat": gg, "lon": d}, device_id_type=MESH)

    for off in OFFS:
        if off != (0, 0):
            tell(bar, g, target(off))
    tell(bar, up, me)
    tell(bar, dn, me)
    for c in loads[:1] + small + loads[1:]:
        c.start()

    def rcopy(src, dst, si, sem, gg, d):
        c = pltpu.make_async_remote_copy(
            src_ref=src, dst_ref=dst, send_sem=sendsem.at[si], recv_sem=sem,
            device_id={"lat": gg, "lon": d}, device_id_type=MESH,
        )
        c.start()

    def send_edges(ph, src):
        for off in OFFS:
            d = target(off)
            rcopy(src.at[pl.ds(2 * d, 2), 6:8], xe.at[ph, me, :, 6:8], 3 * ph + 1, fesem.at[ph, 0], up, d)
            rcopy(src.at[pl.ds(2 * d, 2), 0:2], xe.at[ph, me, :, 0:2], 3 * ph + 2, fesem.at[ph, 1], dn, d)

    def send_main(ph, src):
        for off in OFFS:
            d = target(off)
            if off != (0, 0):
                rcopy(src.at[pl.ds(2 * d, 2)], xm.at[ph, me], 3 * ph, fmsem.at[ph], g, d)
        xm[ph, pl.ds(me, 1)] = src[pl.ds(2 * me, 2)][None]

    def wait15(buf, sem):
        pltpu.make_async_copy(buf.at[pl.ds(0, 15)], buf.at[pl.ds(0, 15)], sem).wait()

    def wait_all(buf, sem):
        pltpu.make_async_copy(buf, buf, sem).wait()

    sub = lax.broadcasted_iota(jnp.int32, (8, 128), 0)
    lane = lax.broadcasted_iota(jnp.int32, (8, 128), 1)

    def tile(read):
        t = jnp.full((8, 128), read(0))
        for r in range(1, 8):
            t = jnp.where(sub == r, read(r), t)
        return t

    valid = jnp.logical_or(
        jnp.logical_and(sub >= 4, jnp.full((8, 128), g) > 0),
        jnp.logical_and(sub < 4, jnp.full((8, 128), g) < NG - 1),
    )

    with jax.named_scope("entry"):
        loads[0].wait()
        for c in small:
            c.wait()
        zc = tile(lambda r: zc_s[r])
        mc = tile(lambda r: mc_s[r])
        mct[...] = mc
        own = lambda ref: tile(lambda r: ref[8 * g + r])
        halo = lambda ref: jnp.where(sub == 0, ref[(8 * g + 8) % 64], ref[(8 * g + 63) % 64])
        pl.semaphore_wait(bar, 17)
        tell(ready, up, me)
        tell(ready, dn, me)
    with jax.named_scope("fwd0"):
        rcopy(mct, mcp, 6, esem.at[0], up, me)
        rcopy(mct, mcn, 6, esem.at[1], dn, me)
        send_main(0, pv)
    with jax.named_scope("home"):
        loads[1].wait()
        e = jnp.zeros((8, 128), F32)
        for k in range(NL):
            uk = uv[k]
            e = jnp.where(lane == k, pltpu.roll(uk, (k + 1) % 128, 1), e)
            e = jnp.where(lane == 32 + k, pltpu.roll(uk, 32 + k, 1), e)
        eu[...] = e
        pl.semaphore_wait(ready, 2)
        send_edges(0, pv)
        rcopy(eu, eul, 7, esem.at[2], g, east)
        rcopy(eu, eur, 7, esem.at[3], g, west)
        loads[2].wait()
        rcopy(vv.at[:, 7:8], ev.at[:, 7:8], 8, esem.at[4], up, me)
        rcopy(vv.at[:, 0:1], ev.at[:, 0:1], 9, esem.at[5], dn, me)

        def factors(cut, mask):
            k1 = lax.broadcasted_iota(jnp.int32, (16, 8, 128), 0)
            k2 = lax.broadcasted_iota(jnp.int32, (16, 8, 128), 2)
            k = k1 + 16 * k2
            kk = jnp.minimum(k, 2048 - k).astype(F32)
            c = cut.astype(F32)[None]
            ratio = c / jnp.maximum(kk, 1.0)
            damped = jnp.logical_and(kk > c, mask[None] > 0)
            return jnp.where(damped, ratio * ratio, 1.0) * (1.0 / 2048.0)

        loads[5].wait()
        loads[6].wait()
        plain = factors(own(cut_s), own(msk_s))
        fb[...] = (-mc[None] * plain).reshape(128, 128)
        for k1 in range(16):
            wave = zc * tw[2, k1 : k1 + 1, :]
            fo[k1 * 8 : k1 * 8 + 8, :] = -wave * plain[k1]
            fd[k1 * 8 : k1 * 8 + 8, :] = wave * wave * plain[k1]

        wait_all(mcp, esem.at[0])
        wait_all(mcn, esem.at[1])
        mch = jnp.where(sub >= 4, mcp[...], mcn[...])
        mch = jnp.where(valid, mch, 0.0)
        rim = -mch[None] * factors(halo(cut_s), halo(msk_s))
        for k1 in range(16):
            row = slice(k1 * 8, k1 * 8 + 8)
            b = fb[row, :]
            above = mc * pltpu.roll(jnp.where(sub == 0, rim[k1], b), 7, 0)
            below = mc * pltpu.roll(jnp.where(sub == 7, rim[k1], b), 1, 0)
            fn[row, :] = above
            fs[row, :] = below
            fd[row, :] = fd[row, :] - (above + below)
    def get_main(ph, d, l):
        x = xm[0, d, l]
        return x + xm[1, d, l] if ph else x

    def get_edge(ph, d, l):
        x = xe[0, d, l]
        x = x + xe[1, d, l] if ph else x
        return x

    def store_spec(t, spec):
        for k1 in range(16):
            r, i = spec[k1]
            tr, ti = tw[0, k1 : k1 + 1, :], tw[1, k1 : k1 + 1, :]
            row = t * 128 + k1 * 8
            lhs[row : row + 8, 0:128] = r * tr - i * ti
            lhs[row : row + 8, 128:256] = r * ti + i * tr

    def big_dot(x):
        high = x.astype(jnp.bfloat16)
        low = (x - high.astype(F32)).astype(jnp.bfloat16)
        one = lambda a, b: jnp.dot(a, b, preferred_element_type=F32)
        return one(jnp.concatenate([high, low, high], axis=1), mat[...])

    def unfold(t):
        x = []
        for k1 in range(16):
            row = t * 128 + k1 * 8
            r, i = res[row : row + 8, 0:128], res[row : row + 8, 128:256]
            tr, ti = tw[0, k1 : k1 + 1, :], tw[1, k1 : k1 + 1, :]
            x.append((r * tr - i * ti, r * ti + i * tr))
        return [(b, a) for a, b in dft16(x)]

    def backward(src, dst, si, sem):
        for off in OFFS:
            d = target(off)
            if off != (0, 0):
                rcopy(src.at[d], dst.at[pl.ds(2 * me, 2)], si, sem, g, d)
        dst[pl.ds(2 * me, 2)] = src[pl.ds(me, 1)][0]

    def wait30(buf, sem):
        pltpu.make_async_copy(buf.at[pl.ds(0, 30)], buf.at[pl.ds(0, 30)], sem).wait()

    def inverse(t, real, imag):
        res[t * 128 : t * 128 + 128, :] = big_dot(jnp.concatenate([imag, real], axis=1))
        return unfold(t)

    def zonal(spec):
        y = inverse(0, -(spec[:, 128:256] * fo[...]), spec[:, 0:128] * fo[...])
        for d in range(16):
            for l in range(2):
                du[d, l] = y[d][l]

    def merid(real, imag):
        y = inverse(1, real, imag)
        for d in range(16):
            for l in range(2):
                dv[d, l] = y[d][l]

    def diverge(ph, real, imag):
        y = inverse(2, real, imag)
        for d in range(16):
            for l in range(2):
                dsend[ph, d, l] = y[d][l]

    def div_spectra(own_spec, edge_spec):
        parts = []
        for half in (0, 128):
            out = []
            for k1 in range(16):
                row = slice(k1 * 8, k1 * 8 + 8)
                o, e = own_spec[row, half : half + 128], edge_spec[row, half : half + 128]
                e = jnp.where(valid, e, 0.0)
                north = pltpu.roll(jnp.where(sub < 2, e, o), 6, 0)
                south = pltpu.roll(jnp.where(sub >= 6, e, o), 2, 0)
                out.append(fd[row, :] * o + fn[row, :] * north + fs[row, :] * south)
            parts.append(jnp.concatenate(out, axis=0))
        return parts

    def dv_spectra(own_spec, edge_spec):
        parts = []
        for half in (0, 128):
            out = []
            for k1 in range(16):
                row = slice(k1 * 8, k1 * 8 + 8)
                o, e = own_spec[row, half : half + 128], edge_spec[row, half : half + 128]
                e = jnp.where(valid, e, 0.0)
                north = pltpu.roll(jnp.where(sub == 0, e, o), 7, 0)
                south = pltpu.roll(jnp.where(sub == 7, e, o), 1, 0)
                out.append(fb[row, :] * (north - south))
            parts.append(jnp.concatenate(out, axis=0))
        return parts

    def wait_edges(ph):
        wait_all(xe.at[ph, :, :, 0:2], fesem.at[ph, 0])
        wait_all(xe.at[ph, :, :, 0:2], fesem.at[ph, 1])

    def fold_main(ph):
        store_spec(0, dft16([(get_main(ph, d, 0), get_main(ph, d, 1)) for d in range(16)]))

    def fold_edge(ph):
        store_spec(1, dft16([(get_edge(ph, d, 0), get_edge(ph, d, 1)) for d in range(16)]))

    def send_du():
        backward(du, ru, 12, bksem.at[2])

    def send_dv():
        backward(dv, rv, 13, bksem.at[3])

    def send_div(ph):
        backward(dsend.at[ph], back.at[ph], 10 + ph, bksem.at[ph])

    def whole(ph):
        fold_main(ph)
        fold_edge(ph)
        spec = big_dot(lhs[...])
        diverge(ph, *div_spectra(spec[0:128], spec[128:256]))
        send_div(ph)
        if ph == SUBSTEPS - 1:
            zonal(spec[0:128])
            send_du()
            merid(*dv_spectra(spec[0:128], spec[128:256]))
            send_dv()

    def parted(ph):
        fold_main(ph)
        spec = big_dot(lhs[0:128, :])
        if ph == SUBSTEPS - 1:
            zonal(spec)
            send_du()
        with jax.named_scope("waite%d" % ph):
            wait_edges(ph)
        with jax.named_scope("edge%d" % ph):
            fold_edge(ph)
            edge_spec = big_dot(lhs[128:256, :])
            diverge(ph, *div_spectra(spec, edge_spec))
            send_div(ph)
            if ph == SUBSTEPS - 1:
                merid(*dv_spectra(spec, edge_spec))
                send_dv()

    def level_part(ph):
        with jax.named_scope("waitm%d" % ph):
            wait15(xm.at[ph], fmsem.at[ph])

        if ph == 0:
            parted(ph)
            return

        @pl.when(par == 0)
        def _():
            wait_edges(ph)
            with jax.named_scope("whole%d" % ph):
                whole(ph)

        @pl.when(par == 1)
        def _():
            parted(ph)

    def column(ph, pin, win, pout, wout):
        ps = [pin[k] - sv[k] * (div0[k] + back[ph, k]) for k in range(NL)]
        vals = []
        pval = jnp.zeros((8, 128), F32)
        for k in range(NL):
            al = a_s[k]
            if k + 1 < NL:
                rhs = win[k] - al * (ps[k + 1] - ps[k])
            else:
                rhs = win[k] + al * ps[k]
            pval = rhs * inv[k] + qq[k] * pval
            vals.append(pval)
        wk = vals[-1]
        for k in range(NL - 1, -1, -1):
            wout[k] = wk
            if k:
                wlow = vals[k - 1] - rat[k - 1] * wk
                pout[k] = ps[k] - sv[k] * (wk - wlow)
                wk = wlow
            else:
                pout[k] = ps[k] - sv[k] * wk

    level_part(0)
    with jax.named_scope("home2"):
        loads[3].wait()
        prev = jnp.zeros((8, 128), F32)
        for k in range(NL):
            al = a_s[k]
            below = al * sv[k]
            above = al * sv[k + 1] if k + 1 < NL else jnp.zeros((8, 128), F32)
            ip = 1.0 / (1.0 + below + above + below * prev)
            prev = -above * ip
            rat[k] = prev
            inv[k] = ip
            qq[k] = below * ip

        wait_all(eul, esem.at[2])
        wait_all(eur, esem.at[3])
        wait_all(ev.at[:, 7:8], esem.at[4])
        wait_all(ev.at[:, 0:1], esem.at[5])
        el, er = eul[...], eur[...]
        for k in range(NL):
            uk, vk = uv[k], vv[k]
            evk = jnp.where(valid, ev[k], 0.0)
            right = jnp.where(lane == 127, pltpu.roll(er, (95 - k) % 128, 1), pltpu.roll(uk, 127, 1))
            left = jnp.where(lane == 0, pltpu.roll(el, (128 - k) % 128, 1), pltpu.roll(uk, 1, 1))
            north = pltpu.roll(jnp.where(sub == 0, evk, vk), 7, 0)
            south = pltpu.roll(jnp.where(sub == 7, evk, vk), 1, 0)
            div0[k] = zc * (right - left) + mc * (north - south)
        loads[4].wait()
    with jax.named_scope("waitb0"):
        wait30(back.at[0], bksem.at[0])
    with jax.named_scope("col0"):
        column(0, pv, wv, p1, w1)
    with jax.named_scope("fwd1"):
        send_edges(1, p1)
        send_main(1, p1)
    level_part(1)
    with jax.named_scope("waitb1"):
        wait30(back.at[1], bksem.at[1])
    with jax.named_scope("col1"):
        column(1, p1, w1, p2, w2)
    with jax.named_scope("fin"):
        wait30(ru, bksem.at[2])
        for k in range(NL):
            uo[k] = ru[k] + uv[k]
        wait30(rv, bksem.at[3])
        for k in range(NL):
            vo[k] = rv[k] + vv[k]
    with jax.named_scope("sends"):
        for ph in range(SUBSTEPS):
            wait15(xm.at[ph], sendsem.at[3 * ph])
            wait_all(xe.at[ph, :, :, 0:2], sendsem.at[3 * ph + 1])
            wait_all(xe.at[ph, :, :, 0:2], sendsem.at[3 * ph + 2])
        wait_all(back.at[0, 0:2], sendsem.at[6])
        wait_all(back.at[0, 0:2], sendsem.at[7])
        wait_all(ev.at[:, 0:1], sendsem.at[8])
        wait_all(ev.at[:, 0:1], sendsem.at[9])
        for i in range(10, 14):
            wait30(ru, sendsem.at[i])

def store(u, v, w, p, uo, vo, wo, po, sem):
    copies = [pltpu.make_async_copy(a, b, sem.at[i]) for i, (a, b) in enumerate([(u, uo), (v, vo), (w, wo), (p, po)])]
    for c in copies:
        c.start()
    for c in copies:
        c.wait()


def solution(mesh):
    mat_np, tw_np = tables()
    field = jax.ShapeDtypeStruct((NL, 8, 128), F32)
    vmem = pl.BlockSpec(memory_space=pltpu.VMEM)
    hbm = pl.BlockSpec(memory_space=pltpu.HBM)
    blk = pltpu.VMEM((NL, 8, 128), F32)
    quad = pltpu.VMEM((2, 16, 2, 8, 128), F32)
    line = pltpu.VMEM((8, 128), F32)
    rows = pltpu.VMEM((384, 256), F32)
    dma = pltpu.SemaphoreType.DMA
    scratch = [
        blk, blk, blk, blk, blk, pltpu.VMEM((768, 256), jnp.bfloat16), pltpu.VMEM((3, 16, 128), F32),
        blk, blk, quad, quad, pltpu.VMEM((256, 256), F32), rows, quad, pltpu.VMEM((2, NL, 8, 128), F32),
        pltpu.VMEM((16, 2, 8, 128), F32), pltpu.VMEM((16, 2, 8, 128), F32), blk, blk,
        blk, blk, blk, blk, line, line, line, blk, line, line, line,
        pltpu.VMEM((128, 128), F32), pltpu.VMEM((128, 128), F32), pltpu.VMEM((128, 128), F32), pltpu.VMEM((128, 128), F32), pltpu.VMEM((128, 128), F32),
        pltpu.SMEM((8,), F32), pltpu.SMEM((8,), F32), pltpu.SMEM((NL,), F32), pltpu.SMEM((64,), jnp.int32), pltpu.SMEM((64,), jnp.int32),
        dma((7,)), dma((5,)), dma((14,)), dma((2,)), dma((2, 2)), dma((4,)), dma((6,)), pltpu.SemaphoreType.REGULAR,
    ]
    call = pl.pallas_call(
        kernel,
        out_shape=(blk,) * 4,
        in_specs=[hbm] * 12,
        out_specs=(vmem,) * 4,
        scratch_shapes=scratch,
        compiler_params=pltpu.CompilerParams(collective_id=0, has_side_effects=True),
    )

    finish = pl.pallas_call(
        store, out_shape=(field,) * 4, in_specs=[vmem] * 4, out_specs=(hbm,) * 4, scratch_shapes=[dma((4,))]
    )

    def hold(*xs):
        return [pltpu.with_memory_space_constraint(o, pltpu.VMEM) for o in call(*xs)]

    def body(u, v, w, p, zc, mc, a, s, cutoff, mask):
        return finish(*hold(zc, mc, a, cutoff, mask, u, v, w, p, s, jnp.asarray(mat_np), jnp.asarray(tw_np)))

    f = P(None, "lat", "lon")
    return jax.shard_map(
        body,
        mesh=mesh,
        in_specs=(f, f, f, f, P("lat"), P("lat"), P(None), f, P(None), P(None)),
        out_specs=(f,) * 4,
        check_vma=False,
    )
```

```python
import math

import jax
import jax.numpy as jnp
import numpy as np
from jax import lax
from jax.experimental import pallas as pl
from jax.experimental.pallas import tpu as pltpu
from jax.sharding import PartitionSpec as P

SUBSTEPS = 2
F32 = jnp.float32
NG = 8
ND = 16
NL = 32
MESH = pl.DeviceIdType.MESH


def tables():
    lane = np.arange(128)
    ang = 2.0 * np.pi * ((lane[:, None] * lane[None, :]) % 128) / 128.0
    c, s = np.cos(ang), np.sin(ang)
    mat = np.block([[c, -s], [s, c]])
    high = mat.astype(np.float32).astype(jnp.bfloat16)
    low = (mat - high.astype(np.float64)).astype(np.float32).astype(jnp.bfloat16)
    mat = np.concatenate([high, high, low])
    tang = 2.0 * np.pi * (np.arange(16)[:, None] * lane[None, :]) / 2048.0
    theta = 2.0 * np.pi * (np.arange(16)[:, None] + 16 * lane[None, :]) / 2048.0
    tw = np.stack([np.cos(tang), -np.sin(tang), 2.0 * np.sin(theta)]).astype(np.float32)
    return mat, tw


def dft4(x):
    (ar, ai), (br, bi), (cr, ci), (dr, di) = x
    sr, si = ar + cr, ai + ci
    tr, ti = ar - cr, ai - ci
    ur, ui = br + dr, bi + di
    vr, vi = br - dr, bi - di
    return [(sr + ur, si + ui), (tr + vi, ti - vr), (sr - ur, si - ui), (tr - vi, ti + vr)]


def dft16(x):
    cols = []
    for n2 in range(4):
        y = dft4([x[4 * n1 + n2] for n1 in range(4)])
        out = []
        for k1 in range(4):
            e = (n2 * k1) % 16
            yr, yi = y[k1]
            if e == 0:
                out.append((yr, yi))
            elif e == 4:
                out.append((yi, -yr))
            else:
                c, s = math.cos(2 * math.pi * e / 16), math.sin(2 * math.pi * e / 16)
                out.append((yr * c + yi * s, yi * c - yr * s))
        cols.append(out)
    res = [None] * 16
    for k1 in range(4):
        z = dft4([cols[n2][k1] for n2 in range(4)])
        for k2 in range(4):
            res[k1 + 4 * k2] = z[k2]
    return res


def hops(off):
    return sum(min(o, 4 - o) for o in off)


OFFS = sorted([(a, b) for a in range(4) for b in range(4)], key=lambda o: -hops(o))


def kernel(
    zc_h, mc_h, a_h, cut_h, msk_h, u_h, v_h, w_h, p_h, s_h, mat_h, tw_h,
    uo, vo, w2, p2,
    uv, vv, wv, pv, sv, mat, tw, p1, w1, xm, xe, lhs, res, dsend, back,
    du, dv, ru, rv, rat, inv, qq, div0, eu, eul, eur, ev, mct, mcp, mcn, fo, fb, fd, fn, fs,
    zc_s, mc_s, a_s, cut_s, msk_s,
    ldsem, smsem, sendsem, fmsem, fesem, bksem, esem, ready,
):
    me = lax.axis_index("lon")
    g = lax.axis_index("lat")
    par = g % 2
    up = (g + 1) % NG
    dn = (g + NG - 1) % NG
    my, mx = me // 4, me % 4
    east = (me + 1) % ND
    west = (me + ND - 1) % ND

    loads = [
        pltpu.make_async_copy(a, b, ldsem.at[i])
        for i, (a, b) in enumerate(
            [(p_h, pv), (u_h, uv), (v_h, vv), (s_h, sv), (w_h, wv), (tw_h, tw), (mat_h, mat)]
        )
    ]
    small = [
        pltpu.make_async_copy(a, b, smsem.at[i])
        for i, (a, b) in enumerate(
            [(zc_h, zc_s), (mc_h, mc_s), (a_h, a_s), (cut_h, cut_s), (msk_h, msk_s)]
        )
    ]
    bar = pltpu.get_barrier_semaphore()

    def target(off):
        return ((my + off[0]) % 4) * 4 + (mx + off[1]) % 4

    def tell(sem, gg, d):
        pl.semaphore_signal(sem, inc=1, device_id={"lat": gg, "lon": d}, device_id_type=MESH)

    for off in OFFS:
        if off != (0, 0):
            tell(bar, g, target(off))
    tell(bar, up, me)
    tell(bar, dn, me)
    for c in loads[:1] + small + loads[1:]:
        c.start()

    def rcopy(src, dst, si, sem, gg, d):
        c = pltpu.make_async_remote_copy(
            src_ref=src, dst_ref=dst, send_sem=sendsem.at[si], recv_sem=sem,
            device_id={"lat": gg, "lon": d}, device_id_type=MESH,
        )
        c.start()

    def edge_up(ph, src, d):
        rcopy(src.at[pl.ds(2 * d, 2), 6:8], xe.at[ph, me, :, 6:8], 3 * ph + 1, fesem.at[ph, 0], up, d)

    def edge_dn(ph, src, d):
        rcopy(src.at[pl.ds(2 * d, 2), 0:2], xe.at[ph, me, :, 0:2], 3 * ph + 2, fesem.at[ph, 1], dn, d)

    def send_edges(ph, src):
        for off in OFFS:
            d = target(off)
            edge_up(ph, src, d)
            edge_dn(ph, src, d)

    def first_edges(src):
        def ups():
            pl.semaphore_wait(ready.at[1], 1)
            for off in OFFS:
                edge_up(0, src, target(off))

        def downs():
            pl.semaphore_wait(ready.at[0], 1)
            for off in OFFS:
                edge_dn(0, src, target(off))

        @pl.when(par == 0)
        def _():
            ups()
            downs()

        @pl.when(par == 1)
        def _():
            downs()
            ups()

    def send_main(ph, src):
        for off in OFFS:
            d = target(off)
            if off != (0, 0):
                rcopy(src.at[pl.ds(2 * d, 2)], xm.at[ph, me], 3 * ph, fmsem.at[ph], g, d)
        xm[ph, pl.ds(me, 1)] = src[pl.ds(2 * me, 2)][None]

    def wait15(buf, sem):
        pltpu.make_async_copy(buf.at[pl.ds(0, 15)], buf.at[pl.ds(0, 15)], sem).wait()

    def wait_all(buf, sem):
        pltpu.make_async_copy(buf, buf, sem).wait()

    sub = lax.broadcasted_iota(jnp.int32, (8, 128), 0)
    lane = lax.broadcasted_iota(jnp.int32, (8, 128), 1)

    def tile(read):
        t = jnp.full((8, 128), read(0))
        for r in range(1, 8):
            t = jnp.where(sub == r, read(r), t)
        return t

    valid = jnp.logical_or(
        jnp.logical_and(sub >= 4, jnp.full((8, 128), g) > 0),
        jnp.logical_and(sub < 4, jnp.full((8, 128), g) < NG - 1),
    )

    with jax.named_scope("entry"):
        loads[0].wait()
        for c in small:
            c.wait()
        zc = tile(lambda r: zc_s[r])
        mc = tile(lambda r: mc_s[r])
        mct[...] = mc
        own = lambda ref: tile(lambda r: ref[8 * g + r])
        halo = lambda ref: jnp.where(sub == 0, ref[(8 * g + 8) % 64], ref[(8 * g + 63) % 64])
        pl.semaphore_wait(bar, 17)
        tell(ready.at[0], up, me)
        tell(ready.at[1], dn, me)
    with jax.named_scope("fwd0"):
        rcopy(mct, mcp, 6, esem.at[0], up, me)
        rcopy(mct, mcn, 6, esem.at[1], dn, me)
        send_main(0, pv)
    with jax.named_scope("home"):
        loads[1].wait()
        e = jnp.zeros((8, 128), F32)
        for k in range(NL):
            uk = uv[k]
            e = jnp.where(lane == k, pltpu.roll(uk, (k + 1) % 128, 1), e)
            e = jnp.where(lane == 32 + k, pltpu.roll(uk, 32 + k, 1), e)
        eu[...] = e
        first_edges(pv)
        rcopy(eu, eul, 7, esem.at[2], g, east)
        rcopy(eu, eur, 7, esem.at[3], g, west)
        loads[2].wait()
        rcopy(vv.at[:, 7:8], ev.at[:, 7:8], 8, esem.at[4], up, me)
        rcopy(vv.at[:, 0:1], ev.at[:, 0:1], 9, esem.at[5], dn, me)

        def factors(cut, mask):
            k1 = lax.broadcasted_iota(jnp.int32, (16, 8, 128), 0)
            k2 = lax.broadcasted_iota(jnp.int32, (16, 8, 128), 2)
            k = k1 + 16 * k2
            kk = jnp.minimum(k, 2048 - k).astype(F32)
            c = cut.astype(F32)[None]
            ratio = c / jnp.maximum(kk, 1.0)
            damped = jnp.logical_and(kk > c, mask[None] > 0)
            return jnp.where(damped, ratio * ratio, 1.0) * (1.0 / 2048.0)

        loads[5].wait()
        loads[6].wait()
        plain = factors(own(cut_s), own(msk_s))
        fb[...] = (-mc[None] * plain).reshape(128, 128)
        for k1 in range(16):
            wave = zc * tw[2, k1 : k1 + 1, :]
            fo[k1 * 8 : k1 * 8 + 8, :] = -wave * plain[k1]
            fd[k1 * 8 : k1 * 8 + 8, :] = wave * wave * plain[k1]

        wait_all(mcp, esem.at[0])
        wait_all(mcn, esem.at[1])
        mch = jnp.where(sub >= 4, mcp[...], mcn[...])
        mch = jnp.where(valid, mch, 0.0)
        rim = -mch[None] * factors(halo(cut_s), halo(msk_s))
        for k1 in range(16):
            row = slice(k1 * 8, k1 * 8 + 8)
            b = fb[row, :]
            above = mc * pltpu.roll(jnp.where(sub == 0, rim[k1], b), 7, 0)
            below = mc * pltpu.roll(jnp.where(sub == 7, rim[k1], b), 1, 0)
            fn[row, :] = above
            fs[row, :] = below
            fd[row, :] = fd[row, :] - (above + below)
    def get_main(ph, d, l):
        x = xm[0, d, l]
        return x + xm[1, d, l] if ph else x

    def get_edge(ph, d, l):
        x = xe[0, d, l]
        x = x + xe[1, d, l] if ph else x
        return x

    def store_spec(t, spec):
        for k1 in range(16):
            r, i = spec[k1]
            tr, ti = tw[0, k1 : k1 + 1, :], tw[1, k1 : k1 + 1, :]
            row = t * 128 + k1 * 8
            lhs[row : row + 8, 0:128] = r * tr - i * ti
            lhs[row : row + 8, 128:256] = r * ti + i * tr

    def big_dot(x):
        high = x.astype(jnp.bfloat16)
        low = (x - high.astype(F32)).astype(jnp.bfloat16)
        one = lambda a, b: jnp.dot(a, b, preferred_element_type=F32)
        return one(jnp.concatenate([high, low, high], axis=1), mat[...])

    def unfold(t):
        x = []
        for k1 in range(16):
            row = t * 128 + k1 * 8
            r, i = res[row : row + 8, 0:128], res[row : row + 8, 128:256]
            tr, ti = tw[0, k1 : k1 + 1, :], tw[1, k1 : k1 + 1, :]
            x.append((r * tr - i * ti, r * ti + i * tr))
        return [(b, a) for a, b in dft16(x)]

    def backward(src, dst, si, sem):
        for off in OFFS:
            d = target(off)
            if off != (0, 0):
                rcopy(src.at[d], dst.at[pl.ds(2 * me, 2)], si, sem, g, d)
        dst[pl.ds(2 * me, 2)] = src[pl.ds(me, 1)][0]

    def wait30(buf, sem):
        pltpu.make_async_copy(buf.at[pl.ds(0, 30)], buf.at[pl.ds(0, 30)], sem).wait()

    def inverse(t, real, imag):
        res[t * 128 : t * 128 + 128, :] = big_dot(jnp.concatenate([imag, real], axis=1))
        return unfold(t)

    def zonal(spec):
        y = inverse(0, -(spec[:, 128:256] * fo[...]), spec[:, 0:128] * fo[...])
        for d in range(16):
            for l in range(2):
                du[d, l] = y[d][l]

    def merid(real, imag):
        y = inverse(1, real, imag)
        for d in range(16):
            for l in range(2):
                dv[d, l] = y[d][l]

    def diverge(ph, real, imag):
        y = inverse(2, real, imag)
        for d in range(16):
            for l in range(2):
                dsend[ph, d, l] = y[d][l]

    def div_spectra(own_spec, edge_spec):
        parts = []
        for half in (0, 128):
            out = []
            for k1 in range(16):
                row = slice(k1 * 8, k1 * 8 + 8)
                o, e = own_spec[row, half : half + 128], edge_spec[row, half : half + 128]
                e = jnp.where(valid, e, 0.0)
                north = pltpu.roll(jnp.where(sub < 2, e, o), 6, 0)
                south = pltpu.roll(jnp.where(sub >= 6, e, o), 2, 0)
                out.append(fd[row, :] * o + fn[row, :] * north + fs[row, :] * south)
            parts.append(jnp.concatenate(out, axis=0))
        return parts

    def dv_spectra(own_spec, edge_spec):
        parts = []
        for half in (0, 128):
            out = []
            for k1 in range(16):
                row = slice(k1 * 8, k1 * 8 + 8)
                o, e = own_spec[row, half : half + 128], edge_spec[row, half : half + 128]
                e = jnp.where(valid, e, 0.0)
                north = pltpu.roll(jnp.where(sub == 0, e, o), 7, 0)
                south = pltpu.roll(jnp.where(sub == 7, e, o), 1, 0)
                out.append(fb[row, :] * (north - south))
            parts.append(jnp.concatenate(out, axis=0))
        return parts

    def wait_edges(ph):
        wait_all(xe.at[ph, :, :, 0:2], fesem.at[ph, 0])
        wait_all(xe.at[ph, :, :, 0:2], fesem.at[ph, 1])

    def fold_main(ph):
        store_spec(0, dft16([(get_main(ph, d, 0), get_main(ph, d, 1)) for d in range(16)]))

    def fold_edge(ph):
        store_spec(1, dft16([(get_edge(ph, d, 0), get_edge(ph, d, 1)) for d in range(16)]))

    def send_du():
        backward(du, ru, 12, bksem.at[2])

    def send_dv():
        backward(dv, rv, 13, bksem.at[3])

    def send_div(ph):
        backward(dsend.at[ph], back.at[ph], 10 + ph, bksem.at[ph])

    def whole(ph):
        fold_main(ph)
        fold_edge(ph)
        spec = big_dot(lhs[...])
        diverge(ph, *div_spectra(spec[0:128], spec[128:256]))
        send_div(ph)
        if ph == SUBSTEPS - 1:
            zonal(spec[0:128])
            send_du()
            merid(*dv_spectra(spec[0:128], spec[128:256]))
            send_dv()

    def parted(ph):
        fold_main(ph)
        spec = big_dot(lhs[0:128, :])
        if ph == SUBSTEPS - 1:
            zonal(spec)
            send_du()
        with jax.named_scope("waite%d" % ph):
            wait_edges(ph)
        with jax.named_scope("edge%d" % ph):
            fold_edge(ph)
            edge_spec = big_dot(lhs[128:256, :])
            diverge(ph, *div_spectra(spec, edge_spec))
            send_div(ph)
            if ph == SUBSTEPS - 1:
                merid(*dv_spectra(spec, edge_spec))
                send_dv()

    def level_part(ph):
        with jax.named_scope("waitm%d" % ph):
            wait15(xm.at[ph], fmsem.at[ph])

        if ph == 0:
            parted(ph)
            return

        @pl.when(par == 0)
        def _():
            wait_edges(ph)
            with jax.named_scope("whole%d" % ph):
                whole(ph)

        @pl.when(par == 1)
        def _():
            parted(ph)

    def column(ph, pin, win, pout, wout):
        ps = [pin[k] - sv[k] * (div0[k] + back[ph, k]) for k in range(NL)]
        vals = []
        pval = jnp.zeros((8, 128), F32)
        for k in range(NL):
            al = a_s[k]
            if k + 1 < NL:
                rhs = win[k] - al * (ps[k + 1] - ps[k])
            else:
                rhs = win[k] + al * ps[k]
            pval = rhs * inv[k] + qq[k] * pval
            vals.append(pval)
        wk = vals[-1]
        for k in range(NL - 1, -1, -1):
            wout[k] = wk
            if k:
                wlow = vals[k - 1] - rat[k - 1] * wk
                pout[k] = ps[k] - sv[k] * (wk - wlow)
                wk = wlow
            else:
                pout[k] = ps[k] - sv[k] * wk

    level_part(0)
    with jax.named_scope("home2"):
        loads[3].wait()
        prev = jnp.zeros((8, 128), F32)
        for k in range(NL):
            al = a_s[k]
            below = al * sv[k]
            above = al * sv[k + 1] if k + 1 < NL else jnp.zeros((8, 128), F32)
            ip = 1.0 / (1.0 + below + above + below * prev)
            prev = -above * ip
            rat[k] = prev
            inv[k] = ip
            qq[k] = below * ip

        wait_all(eul, esem.at[2])
        wait_all(eur, esem.at[3])
        wait_all(ev.at[:, 7:8], esem.at[4])
        wait_all(ev.at[:, 0:1], esem.at[5])
        el, er = eul[...], eur[...]
        for k in range(NL):
            uk, vk = uv[k], vv[k]
            evk = jnp.where(valid, ev[k], 0.0)
            right = jnp.where(lane == 127, pltpu.roll(er, (95 - k) % 128, 1), pltpu.roll(uk, 127, 1))
            left = jnp.where(lane == 0, pltpu.roll(el, (128 - k) % 128, 1), pltpu.roll(uk, 1, 1))
            north = pltpu.roll(jnp.where(sub == 0, evk, vk), 7, 0)
            south = pltpu.roll(jnp.where(sub == 7, evk, vk), 1, 0)
            div0[k] = zc * (right - left) + mc * (north - south)
        loads[4].wait()
    with jax.named_scope("waitb0"):
        wait30(back.at[0], bksem.at[0])
    with jax.named_scope("col0"):
        column(0, pv, wv, p1, w1)
    with jax.named_scope("fwd1"):
        send_edges(1, p1)
        send_main(1, p1)
    level_part(1)
    with jax.named_scope("waitb1"):
        wait30(back.at[1], bksem.at[1])
    with jax.named_scope("col1"):
        column(1, p1, w1, p2, w2)
    with jax.named_scope("fin"):
        wait30(ru, bksem.at[2])
        for k in range(NL):
            uo[k] = ru[k] + uv[k]
        wait30(rv, bksem.at[3])
        for k in range(NL):
            vo[k] = rv[k] + vv[k]
    with jax.named_scope("sends"):
        for ph in range(SUBSTEPS):
            wait15(xm.at[ph], sendsem.at[3 * ph])
            wait_all(xe.at[ph, :, :, 0:2], sendsem.at[3 * ph + 1])
            wait_all(xe.at[ph, :, :, 0:2], sendsem.at[3 * ph + 2])
        wait_all(back.at[0, 0:2], sendsem.at[6])
        wait_all(back.at[0, 0:2], sendsem.at[7])
        wait_all(ev.at[:, 0:1], sendsem.at[8])
        wait_all(ev.at[:, 0:1], sendsem.at[9])
        for i in range(10, 14):
            wait30(ru, sendsem.at[i])

def store(u, v, w, p, uo, vo, wo, po, sem):
    copies = [pltpu.make_async_copy(a, b, sem.at[i]) for i, (a, b) in enumerate([(u, uo), (v, vo), (w, wo), (p, po)])]
    for c in copies:
        c.start()
    for c in copies:
        c.wait()


def solution(mesh):
    mat_np, tw_np = tables()
    field = jax.ShapeDtypeStruct((NL, 8, 128), F32)
    vmem = pl.BlockSpec(memory_space=pltpu.VMEM)
    hbm = pl.BlockSpec(memory_space=pltpu.HBM)
    blk = pltpu.VMEM((NL, 8, 128), F32)
    quad = pltpu.VMEM((2, 16, 2, 8, 128), F32)
    line = pltpu.VMEM((8, 128), F32)
    rows = pltpu.VMEM((384, 256), F32)
    dma = pltpu.SemaphoreType.DMA
    scratch = [
        blk, blk, blk, blk, blk, pltpu.VMEM((768, 256), jnp.bfloat16), pltpu.VMEM((3, 16, 128), F32),
        blk, blk, quad, quad, pltpu.VMEM((256, 256), F32), rows, quad, pltpu.VMEM((2, NL, 8, 128), F32),
        pltpu.VMEM((16, 2, 8, 128), F32), pltpu.VMEM((16, 2, 8, 128), F32), blk, blk,
        blk, blk, blk, blk, line, line, line, blk, line, line, line,
        pltpu.VMEM((128, 128), F32), pltpu.VMEM((128, 128), F32), pltpu.VMEM((128, 128), F32), pltpu.VMEM((128, 128), F32), pltpu.VMEM((128, 128), F32),
        pltpu.SMEM((8,), F32), pltpu.SMEM((8,), F32), pltpu.SMEM((NL,), F32), pltpu.SMEM((64,), jnp.int32), pltpu.SMEM((64,), jnp.int32),
        dma((7,)), dma((5,)), dma((14,)), dma((2,)), dma((2, 2)), dma((4,)), dma((6,)), pltpu.SemaphoreType.REGULAR((2,)),
    ]
    call = pl.pallas_call(
        kernel,
        out_shape=(blk,) * 4,
        in_specs=[hbm] * 12,
        out_specs=(vmem,) * 4,
        scratch_shapes=scratch,
        compiler_params=pltpu.CompilerParams(collective_id=0, has_side_effects=True),
    )

    finish = pl.pallas_call(
        store, out_shape=(field,) * 4, in_specs=[vmem] * 4, out_specs=(hbm,) * 4, scratch_shapes=[dma((4,))]
    )

    def hold(*xs):
        return [pltpu.with_memory_space_constraint(o, pltpu.VMEM) for o in call(*xs)]

    def body(u, v, w, p, zc, mc, a, s, cutoff, mask):
        return finish(*hold(zc, mc, a, cutoff, mask, u, v, w, p, s, jnp.asarray(mat_np), jnp.asarray(tw_np)))

    f = P(None, "lat", "lon")
    return jax.shard_map(
        body,
        mesh=mesh,
        in_specs=(f, f, f, f, P("lat"), P("lat"), P(None), f, P(None), P(None)),
        out_specs=(f,) * 4,
        check_vma=False,
    )
```
